32 devices in a mesh: dp: 8 (over z, core), tp: 4 (over y, x).
Axes of the slice: x: 2, y: 2, z: 4, core: 2. Of those that a mesh axis runs over, the one named last changes fastest.
Arguments:
- hidden: bfloat16 [384, 4096], P('dp'), may hold values from -6 to 6
- w_qkv: bfloat16 [4096, 4608], P('dp', 'tp'), may hold values from -0.09375 to 0.09375
- w_out: bfloat16 [4096, 4096], P('tp', 'dp'), may hold values from -0.125 to 0.125
- norm_gain: float32 [4096], replicated, may hold values from 0.5 to 1.5
- kv_cache: bfloat16 [384, 2, 128, 256], P(('dp', 'tp')), may hold values from -110 to 110
- lengths: int32 [384], P(('dp', 'tp')), may hold values from 1 to 127, as said below
Outputs:
- residual_out: bfloat16 [384, 4096], P('dp', 'tp')
- scaled: bfloat16 [384, 4096], P('dp', 'tp')
- row_scale: float32 [384], P('dp')
The draws below stay inside these ranges and needn't reach their ends.
Inputs may be any that keep to these rules, and one draw needn't show every extreme that they name: `lengths`: every sequence has 1 to 127 live positions; among each device's 12 sequences one has exactly 127.
All inputs are finite; a program needn't handle non-finite values.
Results may differ from the reference program's by a relative error of at most 0.015.
Values may be sent and summed in bfloat16 or wider, within the bound.
A program may use at most 64 MiB of HBM per device.

```python
import jax
import jax.numpy as jnp
from jax import lax

D = 4096
KVH = 2
HD = 128
HEADS = 32
SEQ_DEV = 12
CTX = 128
QKV = 4608
ATT = 4096
TOTAL_SEQ = 384
N_TP = 4


def draw_kv_cache(key, part):
    shape = (TOTAL_SEQ, KVH, CTX, 2 * HD)
    key_main = jax.random.fold_in(key, 11)
    values = jnp.clip(jax.random.normal(key_main, shape, jnp.float32), -6.0, 6.0)
    return values.astype(jnp.bfloat16)


def draw_lengths(key, part):
    key_base = jax.random.fold_in(key, 21)
    key_pick = jax.random.fold_in(key, 22)
    base = jax.random.randint(key_base, (TOTAL_SEQ,), 1, CTX)
    picked = jax.random.randint(key_pick, (TOTAL_SEQ // SEQ_DEV,), 0, SEQ_DEV)
    slots = jnp.arange(TOTAL_SEQ) % SEQ_DEV
    owners = jnp.arange(TOTAL_SEQ) // SEQ_DEV
    return jnp.where(slots == picked[owners], CTX - 1, base).astype(jnp.int32)


def with_spikes(entries, stream_key, source, target, blocks, factor):
    def block_of(position):
        return (jnp.arange(entries.shape[position]) // (entries.shape[position] // blocks)).reshape((-1,) + (1,) * (entries.ndim - 1 - position))

    first = jax.random.permutation(stream_key, blocks)[block_of(target)]
    other_side = (block_of(target) + blocks // 2) % blocks
    return jnp.where((block_of(source) == first) | (block_of(source) == other_side), factor * entries, entries)


def levels(stream_key, dims, shards, smallest, high):
    level = 1.0
    for axis_at, blocks in shards:
        heights = jax.random.uniform(jax.random.fold_in(jax.random.fold_in(stream_key, 6), axis_at), (blocks,), jnp.float32, smallest / len(shards), high / len(shards))
        level = level * jnp.repeat(jnp.exp(heights), dims[axis_at] // blocks).reshape((-1,) + (1,) * (len(dims) - 1 - axis_at))
    return level


def normal_values(rng, shape, spread, bound, cuts=(), kind=jnp.bfloat16):
    gain = levels(rng, shape, cuts, -0.22, 0.18) if cuts else 1.0
    result = jax.random.normal(rng, shape, jnp.float32) * spread * gain
    return jnp.minimum(jnp.maximum(result, -bound), bound).astype(kind)


def noise_with(key, shape, scale, most, shards, heavy, kind=jnp.bfloat16):
    values = scale * jax.random.normal(key, shape, jnp.float32)
    if shards:
        values = values * levels(key, shape, shards, -0.22, 0.18)
    return jnp.clip(with_spikes(values, jax.random.fold_in(key, 3), *heavy), -most, most).astype(kind)


def setup_inputs(seed: int = 0) -> dict:
    streams_of = jax.random.split(jax.random.key(seed), 7)
    hidden = normal_values(streams_of[0], (TOTAL_SEQ, D), 1.0, 6.0, ((0, 8),))
    w_qkv = normal_values(streams_of[1], (D, QKV), D ** -0.5, 0.09375, ((0, 8), (1, 4)))
    w_out = noise_with(streams_of[2], (ATT, D), ATT ** -0.5, 0.125, ((0, 4), (1, 8)), (0, 1, 8, 2.0))
    norm_gain = jnp.clip(1.0 + 0.1 * jax.random.normal(streams_of[3], (D,), jnp.float32), 0.5, 1.5)
    kv_cache = draw_kv_cache(jax.random.fold_in(streams_of[6], 71), 0)
    lengths = draw_lengths(jax.random.fold_in(streams_of[6], 71), 0)
    return {"hidden": hidden, "w_qkv": w_qkv, "w_out": w_out, "norm_gain": norm_gain, "kv_cache": kv_cache, "lengths": lengths}


def rope(values, positions):
    half = values.shape[-1] // 2
    freqs = 1000000.0 ** (-2.0 * jnp.arange(half, dtype=jnp.float32) / values.shape[-1])
    angle = positions[..., None] * freqs
    cosine = jnp.cos(angle)
    sine = jnp.sin(angle)
    first = values[..., :half]
    second = values[..., half:]
    return jnp.concatenate([first * cosine - second * sine, second * cosine + first * sine], axis=-1)

def attend(query, key_new, value_new, cache, live):
    count = query.shape[0]
    groups = HEADS // KVH
    q_grp = query.reshape(count, KVH, groups, HD).astype(jnp.float32)
    keys = cache[..., :HD].astype(jnp.float32)
    vals = cache[..., HD:].astype(jnp.float32)
    scale = 1.0 / HD ** 0.5
    scores = jnp.einsum('nkgd,nkpd->nkgp', q_grp, keys) * scale
    own = jnp.einsum('nkgd,nkd->nkg', q_grp, key_new.astype(jnp.float32)) * scale
    valid = (jnp.arange(CTX)[None, :] < live[:, None])[:, None, None, :]
    scores = jnp.where(valid, scores, jnp.float32(-1e+30))
    top = jnp.maximum(lax.optimization_barrier(jnp.max(scores, axis=-1)), own)
    probs = jnp.where(valid, jnp.exp(scores - top[..., None]), jnp.float32(0.0))
    own_prob = jnp.exp(own - top)
    denom = lax.optimization_barrier(jnp.sum(probs, axis=-1)) + own_prob
    weights = (probs / denom[..., None]).astype(jnp.bfloat16)
    own_weight = (own_prob / denom).astype(jnp.bfloat16)
    mixed = jnp.einsum('nkgp,nkpd->nkgd', weights.astype(jnp.float32), vals)
    mixed = mixed + own_weight.astype(jnp.float32)[..., None] * value_new.astype(jnp.float32)[:, :, None, :]
    return mixed.reshape(count, ATT).astype(jnp.bfloat16)

def reference(hidden, w_qkv, w_out, norm_gain, kv_cache, lengths):
    total_rows = hidden.shape[0]
    qkv = jnp.dot(hidden, w_qkv, preferred_element_type=jnp.float32).astype(jnp.bfloat16)
    positions = lengths.astype(jnp.float32)[:, None]
    query = qkv[:, :ATT].reshape(total_rows, HEADS, HD).astype(jnp.float32)
    key_new = qkv[:, ATT:ATT + KVH * HD].reshape(total_rows, KVH, HD).astype(jnp.float32)
    value_new = qkv[:, ATT + KVH * HD:].reshape(total_rows, KVH, HD)
    query = rope(query, positions).astype(jnp.bfloat16)
    key_new = rope(key_new, positions).astype(jnp.bfloat16)
    blocks = total_rows // SEQ_DEV

    def one_block(index):
        start = (index * SEQ_DEV).astype(jnp.int32)
        q_blk = lax.dynamic_slice_in_dim(query, start, SEQ_DEV, 0)
        k_blk = lax.dynamic_slice_in_dim(key_new, start, SEQ_DEV, 0)
        v_blk = lax.dynamic_slice_in_dim(value_new, start, SEQ_DEV, 0)
        c_blk = lax.dynamic_slice_in_dim(kv_cache, start, SEQ_DEV, 0)
        l_blk = lax.dynamic_slice_in_dim(lengths, start, SEQ_DEV, 0)
        return attend(q_blk, k_blk, v_blk, c_blk, l_blk)
    attn = lax.map(one_block, jnp.arange(blocks, dtype=jnp.int32)).reshape(total_rows, ATT)
    width = ATT // N_TP
    total = jnp.zeros((total_rows, D), jnp.float32)
    for shard in range(N_TP):
        partial_term = jnp.dot(attn[:, shard * width:(shard + 1) * width], w_out[shard * width:(shard + 1) * width, :], preferred_element_type=jnp.float32)
        total = total + partial_term.astype(jnp.bfloat16).astype(jnp.float32)
    resid = hidden.astype(jnp.float32) + total
    residual_out = resid.astype(jnp.bfloat16)
    inverse = lax.rsqrt(lax.optimization_barrier(jnp.mean(resid * resid, axis=-1, keepdims=True)) + 1e-06)
    normed = resid * norm_gain[None, :] * inverse
    row_scale = (lax.optimization_barrier(jnp.max(jnp.abs(normed), axis=-1)) + 1e-06) / 448.0
    scaled = (normed / row_scale[:, None]).astype(jnp.bfloat16)
    return (residual_out, scaled, row_scale)
```

```python
import functools

import jax
import jax.numpy as jnp
from jax import lax
from jax.experimental import pallas as pl
from jax.experimental.pallas import tpu as pltpu
from jax.sharding import PartitionSpec as P


def rope(values, positions):
    half = values.shape[-1] // 2
    freqs = 1000000.0 ** (-2.0 * jnp.arange(half, dtype=jnp.float32) / values.shape[-1])
    angle = positions[..., None] * freqs
    cosine = jnp.cos(angle)
    sine = jnp.sin(angle)
    first = values[..., :half]
    second = values[..., half:]
    return jnp.concatenate(
        [first * cosine - second * sine, second * cosine + first * sine], axis=-1
    )


def shards(hidden, w_qkv, w_out, norm_gain, kv_cache, lengths):
    seq_dev = kv_cache.shape[0]
    kv_heads = kv_cache.shape[1]
    head_size = kv_cache.shape[3] // 2
    tp_count = lax.axis_size("tp")
    w_cols = lax.all_gather(w_qkv, "dp", axis=0, tiled=True)
    qkv_part = jnp.dot(hidden, w_cols, preferred_element_type=jnp.float32)
    mine = lax.all_to_all(
        qkv_part.astype(jnp.bfloat16), "tp", split_axis=0, concat_axis=1, tiled=True
    )
    att_width = w_out.shape[0] * tp_count
    heads = att_width // head_size
    groups = heads // kv_heads
    positions = lengths.astype(jnp.float32)[:, None]
    query = rope(
        mine[:, :att_width].reshape(seq_dev, heads, head_size).astype(jnp.float32), positions
    ).astype(jnp.bfloat16)
    key_new = rope(
        mine[:, att_width : att_width + kv_heads * head_size]
        .reshape(seq_dev, kv_heads, head_size)
        .astype(jnp.float32),
        positions,
    ).astype(jnp.bfloat16)
    value_new = mine[:, att_width + kv_heads * head_size :].reshape(seq_dev, kv_heads, head_size)
    q_grp = query.reshape(seq_dev, kv_heads, groups, head_size)
    keys = kv_cache[..., :head_size]
    vals = kv_cache[..., head_size:]
    scale = 1.0 / head_size**0.5
    scores = jnp.einsum("nkgd,nkpd->nkgp", q_grp, keys, preferred_element_type=jnp.float32) * scale
    own = jnp.einsum("nkgd,nkd->nkg", q_grp, key_new, preferred_element_type=jnp.float32) * scale
    valid = (jnp.arange(kv_cache.shape[2])[None, :] < lengths[:, None])[:, None, None, :]
    scores = jnp.where(valid, scores, jnp.float32(-1e30))
    top = jnp.maximum(jnp.max(scores, axis=-1), own)
    probs = jnp.where(valid, jnp.exp(scores - top[..., None]), jnp.float32(0.0))
    own_prob = jnp.exp(own - top)
    denom = jnp.sum(probs, axis=-1) + own_prob
    weights = (probs / denom[..., None]).astype(jnp.bfloat16)
    own_weight = (own_prob / denom).astype(jnp.bfloat16)
    mixed = jnp.einsum("nkgp,nkpd->nkgd", weights, vals, preferred_element_type=jnp.float32)
    mixed = (
        mixed
        + own_weight.astype(jnp.float32)[..., None] * value_new.astype(jnp.float32)[:, :, None, :]
    )
    attn = mixed.reshape(seq_dev, att_width).astype(jnp.bfloat16)
    heads_part = lax.all_to_all(attn, "tp", split_axis=1, concat_axis=0, tiled=True)
    terms = jnp.dot(
        heads_part,
        lax.all_gather(w_out, "dp", axis=1, tiled=True),
        preferred_element_type=jnp.float32,
    )
    width = terms.shape[1]
    share = width // tp_count
    offset = lax.axis_index("tp") * share
    summed = lax.psum_scatter(
        terms.astype(jnp.bfloat16), "tp", scatter_dimension=1, tiled=True
    ).astype(jnp.float32)
    hidden_mine = lax.dynamic_slice_in_dim(hidden, offset, share, 1).astype(jnp.float32)
    gain_mine = lax.dynamic_slice_in_dim(norm_gain, offset, share, 0)
    resid_mine = hidden_mine + summed
    weighted = resid_mine * gain_mine[None, :]
    squares = lax.psum(jnp.sum(resid_mine * resid_mine, axis=-1), "tp")
    peak = lax.pmax(jnp.max(jnp.abs(weighted), axis=-1), "tp")
    inverse = lax.rsqrt(squares / width + 1e-06)
    normed_mine = weighted * inverse[:, None]
    row_scale = (peak * inverse + 1e-06) / 448.0
    residual_out = resid_mine.astype(jnp.bfloat16)
    scaled = (normed_mine / row_scale[:, None]).astype(jnp.bfloat16)
    return (residual_out, scaled, row_scale)


F32 = jnp.float32
BF16 = jnp.bfloat16
MESH = pl.DeviceIdType.MESH


def send(src, dst, send_sem, recv_sem, where):
    copy = pltpu.make_async_remote_copy(
        src_ref=src, dst_ref=dst, send_sem=send_sem, recv_sem=recv_sem,
        device_id=where, device_id_type=MESH,
    )
    copy.start()
    return copy


def layer(
    n_dp, n_tp,
    hidden, w_qkv, w_out, gain, cache, lens,
    resid_out, scaled_out, scale_out,
    h_all, w1, w2, kv, hid, hid32, p_send, p_recv, r_acc, r_send, r_recv, mine32,
    t1_send, t1_recv, q_rows, k_rows, v_rows, l_rows, s_rows, a_rows,
    t2_send, t2_recv, b_rows, ag, mm, mq, t3_send, t3_recv, f_send, f_recv,
    o_send, o_recv, c_send, c_recv, fin,
    loc_sem, h_s, h_r, p_s, p_r, r_s, r_r, t1_s, t1_r, t2_s, t2_r,
    g_s, g_r, x_s, t3_s, t3_r, f_s, f_r, o_s, o_r, c_s, c_r,
):
    dp = lax.axis_index("dp")
    tp = lax.axis_index("tp")
    core = lax.rem(dp, 2)
    chip = dp // 2
    other = 1 - core
    partner = chip * 2 + other
    n_chip = n_dp // 2
    rows = hidden.shape[0]
    seqs = rows // n_tp
    depth = w_qkv.shape[0]
    ocols = w_out.shape[1]
    owide = resid_out.shape[1]
    kvh = cache.shape[1]
    ctx = cache.shape[2]
    hd = cache.shape[3] // 2
    heads = (w_out.shape[0] * n_tp) // hd
    groups = heads // kvh
    per = w_qkv.shape[1] // hd
    per_out = w_out.shape[0] // hd
    width = hidden.shape[1]

    own_h = pltpu.make_async_copy(
        hidden.at[:, pl.ds(pl.multiple_of(dp * depth, depth), depth)], h_all.at[core, chip], loc_sem.at[0])
    own_h.start()
    load_w1 = pltpu.make_async_copy(w_qkv, w1, loc_sem.at[1])
    load_w1.start()

    barrier = pltpu.get_barrier_semaphore()
    for d in range(1, n_dp):
        pl.semaphore_signal(barrier, inc=1, device_id={"dp": lax.rem(dp + d, n_dp)}, device_id_type=MESH)
    for d in range(1, n_tp):
        pl.semaphore_signal(barrier, inc=1, device_id={"tp": lax.rem(tp + d, n_tp)}, device_id_type=MESH)
    pl.semaphore_wait(barrier, n_dp + n_tp - 2)

    pending = []
    for d in range(1, n_dp):
        peer = lax.rem(dp + d, n_dp)
        pending.append(send(
            hidden.at[:, pl.ds(pl.multiple_of(peer * depth, depth), depth)],
            h_all.at[core, chip], h_s.at[peer], h_r.at[dp], {"dp": peer}))
    load_kv = pltpu.make_async_copy(cache, kv, loc_sem.at[2])
    load_kv.start()
    load_w2 = pltpu.make_async_copy(w_out, w2, loc_sem.at[3])
    load_w2.start()
    load_hid = pltpu.make_async_copy(hidden, hid, loc_sem.at[4])
    load_hid.start()

    row_i = lax.broadcasted_iota(jnp.int32, (seqs, hd), 0)
    lane_i = lax.broadcasted_iota(jnp.int32, (seqs, hd), 1)
    live = jnp.zeros((seqs, hd), jnp.int32)
    for n in range(seqs):
        live = jnp.where(row_i == n, lens[n], live)
    half = hd // 2
    low = lane_i < half
    index = jnp.where(low, lane_i, lane_i - half).astype(F32)
    freqs = jnp.exp(index * F32(-2.0 * 13.815510557964274 / hd))
    angle = live.astype(F32) * freqs
    cosine = jnp.cos(angle)
    sine = jnp.where(low, -jnp.sin(angle), jnp.sin(angle))
    for h in range(heads):
        l_rows[pl.ds(h, seqs, stride=heads), :] = live.astype(F32)
    load_hid.wait()
    hid32[...] = hid[...].astype(F32)

    def recv_h(peer):
        pltpu.make_async_remote_copy(
            src_ref=h_all.at[core, chip], dst_ref=h_all.at[lax.rem(peer, 2), peer // 2],
            send_sem=h_s.at[peer], recv_sem=h_r.at[peer],
            device_id={"dp": peer}, device_id_type=MESH).wait_recv()

    own_h.wait()
    load_w1.wait()
    for d in range(n_chip):
        recv_h(2 * d + other)
    part = jnp.dot(h_all[other].reshape(n_chip * rows, depth), w1[...], preferred_element_type=F32)
    p_send[...] = part.astype(BF16).reshape(p_send.shape)
    swap = send(p_send, p_recv, p_s, p_r, {"dp": partner})
    pending.append(swap)
    for d in range(1, n_chip):
        recv_h(2 * lax.rem(chip + d, n_chip) + core)
    part = jnp.dot(h_all[core].reshape(n_chip * rows, depth), w1[...], preferred_element_type=F32)
    r_acc[...] = part.reshape(r_acc.shape)
    swap.wait_recv()
    for d in range(1, n_chip):
        to = lax.rem(chip + d, n_chip)
        r_send[to] = (r_acc[to] + p_recv[to].astype(F32)).astype(BF16)
        pending.append(send(r_send.at[to], r_recv.at[chip], r_s.at[to], r_r.at[chip], {"dp": to * 2 + core}))
    total = r_acc[chip] + p_recv[chip].astype(F32)
    for d in range(1, n_chip):
        who = lax.rem(chip + d, n_chip)
        pltpu.make_async_remote_copy(
            src_ref=r_send.at[who], dst_ref=r_recv.at[who], send_sem=r_s.at[who], recv_sem=r_r.at[who],
            device_id={"dp": who * 2 + core}, device_id_type=MESH).wait_recv()
        total = total + r_recv[who].astype(F32)
    mine32[...] = total

    def exchange(src, dst, s_sem, r_sem, fill):
        for q in range(n_tp):
            fill(q)
        keep = pltpu.make_async_copy(src.at[tp], dst.at[tp], r_sem.at[tp])
        keep.start()
        sent = []
        for d in range(1, n_tp):
            peer = lax.rem(tp + d, n_tp)
            sent.append(send(src.at[peer], dst.at[tp], s_sem.at[peer], r_sem.at[tp], {"tp": peer}))
        keep.wait()
        for d in range(1, n_tp):
            peer = lax.rem(tp + d, n_tp)
            pltpu.make_async_remote_copy(
                src_ref=src.at[peer], dst_ref=dst.at[peer], send_sem=s_sem.at[peer], recv_sem=r_sem.at[peer],
                device_id={"tp": peer}, device_id_type=MESH).wait_recv()
        return sent

    def fill1(q):
        t1_send[q] = mine32[q * seqs : (q + 1) * seqs, :].astype(BF16)

    pending += exchange(t1_send, t1_recv, t1_s, t1_r, fill1)

    def head(h):
        return t1_recv[h // per, :, (h % per) * hd : (h % per + 1) * hd].astype(F32)

    def turn(x):
        return (x * cosine + pltpu.roll(x, half, 1) * sine).astype(BF16).astype(F32)

    for h in range(heads):
        q_rows[pl.ds(h, seqs, stride=heads), :] = turn(head(h))
    for k in range(kvh):
        key_new = turn(head(heads + k))
        value_new = head(heads + kvh + k)
        for g in range(groups):
            k_rows[pl.ds(k * groups + g, seqs, stride=heads), :] = key_new
            v_rows[pl.ds(k * groups + g, seqs, stride=heads), :] = value_new
    load_kv.wait()
    for n in range(seqs):
        for k in range(kvh):
            at = (n * kvh + k) * groups
            s_rows[at : at + groups, :] = lax.dot_general(
                q_rows[at : at + groups, :].astype(BF16), kv[n, k, :, :hd],
                (((1,), (1,)), ((), ())), preferred_element_type=F32)
    factor = F32(1.0 / hd**0.5)
    pos = lax.broadcasted_iota(jnp.int32, (seqs * heads, ctx), 1).astype(F32)
    valid = pos < l_rows[...]
    scores = jnp.where(valid, s_rows[...] * factor, F32(-1e30))
    own = jnp.sum(q_rows[...] * k_rows[...], axis=1, keepdims=True) * factor
    top = jnp.maximum(jnp.max(scores, axis=1, keepdims=True), own)
    probs = jnp.where(valid, jnp.exp(scores - top), F32(0.0))
    own_prob = jnp.exp(own - top)
    denom = jnp.sum(probs, axis=1, keepdims=True) + own_prob
    s_rows[...] = probs / denom
    own_weight = (own_prob / denom).astype(BF16).astype(F32)
    v_rows[...] = own_weight * v_rows[...]
    for n in range(seqs):
        for k in range(kvh):
            at = (n * kvh + k) * groups
            a_rows[at : at + groups, :] = jnp.dot(
                s_rows[at : at + groups, :].astype(BF16), kv[n, k, :, hd:],
                preferred_element_type=F32) + v_rows[at : at + groups, :]

    def fill2(q):
        for e in range(per_out):
            t2_send[q, :, e * hd : (e + 1) * hd] = a_rows[
                pl.ds(q * per_out + e, seqs, stride=heads), :].astype(BF16)

    pending += exchange(t2_send, t2_recv, t2_s, t2_r, fill2)
    for q in range(n_tp):
        b_rows[q * seqs : (q + 1) * seqs, :] = t2_recv[q].astype(F32)
    ag[core, chip] = b_rows[...].astype(BF16)
    for d in range(1, n_chip):
        to = lax.rem(chip + d, n_chip)
        pending.append(send(ag.at[core, chip], ag.at[core, chip], g_s.at[to], g_r.at[core, chip],
                            {"dp": to * 2 + core}))
    pending.append(send(ag.at[core, chip], ag.at[core, chip], x_s.at[chip], g_r.at[core, chip], {"dp": partner}))

    def recv_g(c, who):
        pltpu.make_async_remote_copy(
            src_ref=ag.at[core, chip], dst_ref=ag.at[c, who], send_sem=x_s.at[chip], recv_sem=g_r.at[c, who],
            device_id={"dp": partner}, device_id_type=MESH).wait_recv()

    for d in range(1, n_chip):
        who = lax.rem(chip + d, n_chip)
        recv_g(core, who)
        pending.append(send(ag.at[core, who], ag.at[core, who], x_s.at[who], g_r.at[core, who], {"dp": partner}))
    load_w2.wait()
    mm[core] = jnp.dot(ag[core].reshape(n_chip * rows, w_out.shape[0]), w2[...],
                       preferred_element_type=F32).reshape(n_chip, rows, ocols)
    for d in range(n_chip):
        recv_g(other, d)
    mm[other] = jnp.dot(ag[other].reshape(n_chip * rows, w_out.shape[0]), w2[...],
                        preferred_element_type=F32).reshape(n_chip, rows, ocols)

    def fill3(q):
        for r in range(n_dp):
            mq[q, r * seqs : (r + 1) * seqs, :] = mm[r % 2, r // 2, q * seqs : (q + 1) * seqs, :]
        t3_send[q] = mq[q].astype(BF16)

    pending += exchange(t3_send, t3_recv, t3_s, t3_r, fill3)
    total = t3_recv[0].astype(F32)
    for q in range(1, n_tp):
        total = total + t3_recv[q].astype(F32)
    mq[0] = total
    for r in range(n_dp):
        f_send[r] = mq[0, r * seqs : (r + 1) * seqs, :].astype(BF16)
    keep = pltpu.make_async_copy(f_send.at[dp], f_recv.at[dp], f_r.at[dp])
    keep.start()
    for d in range(1, n_dp):
        peer = lax.rem(dp + d, n_dp)
        pending.append(send(f_send.at[peer], f_recv.at[dp], f_s.at[peer], f_r.at[dp], {"dp": peer}))
    keep.wait()
    for d in range(1, n_dp):
        peer = lax.rem(dp + d, n_dp)
        pltpu.make_async_remote_copy(
            src_ref=f_send.at[peer], dst_ref=f_recv.at[peer], send_sem=f_s.at[peer], recv_sem=f_r.at[peer],
            device_id={"dp": peer}, device_id_type=MESH).wait_recv()
    for r in range(n_dp):
        block = slice(r * ocols, (r + 1) * ocols)
        mine = hid32[0:seqs, block]
        for q in range(1, n_tp):
            mine = jnp.where(tp == q, hid32[q * seqs : (q + 1) * seqs, block], mine)
        fin[:, block] = mine + f_recv[r].astype(F32)
    resid = fin[...]
    inverse = lax.rsqrt(jnp.sum(resid * resid, axis=1, keepdims=True) / width + F32(1e-06))
    weighted = resid * gain[...]
    peak = jnp.max(jnp.abs(weighted), axis=1, keepdims=True)
    scale = (peak * inverse + F32(1e-06)) / F32(448.0)
    scaled = (weighted * (inverse / scale)).astype(BF16)
    for q in range(n_tp):
        o_send[q, 0] = resid[:, q * owide : (q + 1) * owide].astype(BF16)
        o_send[q, 1] = scaled[:, q * owide : (q + 1) * owide]
    spread = jnp.where(lane_i == row_i + tp * seqs, jnp.broadcast_to(scale, lane_i.shape), F32(0.0))
    c_send[...] = jnp.broadcast_to(jnp.sum(spread, axis=0, keepdims=True), c_send.shape)
    for d in range(1, n_tp):
        peer = lax.rem(tp + d, n_tp)
        pending.append(send(c_send, c_recv.at[tp], c_s.at[peer], c_r.at[tp], {"tp": peer}))
    pending += exchange(o_send, o_recv, o_s, o_r, lambda q: None)
    scales = c_send[...]
    for d in range(1, n_tp):
        peer = lax.rem(tp + d, n_tp)
        pltpu.make_async_remote_copy(
            src_ref=c_send, dst_ref=c_recv.at[peer], send_sem=c_s.at[peer], recv_sem=c_r.at[peer],
            device_id={"tp": peer}, device_id_type=MESH).wait_recv()
        scales = scales + c_recv[peer]
    scale_out[...] = scales
    for part, out in ((0, resid_out), (1, scaled_out)):
        for q in range(n_tp):
            b_rows[q * seqs : (q + 1) * seqs, :] = o_recv[q, part].astype(F32)
        out[...] = b_rows[...].astype(BF16)
    for copy in pending:
        copy.wait_send()


def fused(n_dp, n_tp, hidden, w_qkv, w_out, norm_gain, kv_cache, lengths):
    rows, width = hidden.shape
    seqs, kvh, ctx, hd2 = kv_cache.shape
    hd = hd2 // 2
    depth, cols = w_qkv.shape
    odepth, ocols = w_out.shape
    heads = odepth * n_tp // hd
    owide = width // n_tp
    chips = n_dp // 2
    vm = pltpu.VMEM
    dma = pltpu.SemaphoreType.DMA
    all_rows = seqs * heads
    scratch = [
        vm((2, chips, rows, depth), BF16), vm((depth, cols), BF16), vm((odepth, ocols), BF16),
        vm(kv_cache.shape, BF16), vm((rows, width), BF16), vm((rows, width), F32),
        vm((chips, rows, cols), BF16), vm((chips, rows, cols), BF16), vm((chips, rows, cols), F32),
        vm((chips, rows, cols), BF16), vm((chips, rows, cols), BF16), vm((rows, cols), F32),
        vm((n_tp, seqs, cols), BF16), vm((n_tp, seqs, cols), BF16),
        vm((all_rows, hd), F32), vm((all_rows, hd), F32), vm((all_rows, hd), F32), vm((all_rows, hd), F32),
        vm((all_rows, ctx), F32), vm((all_rows, hd), F32),
        vm((n_tp, seqs, odepth), BF16), vm((n_tp, seqs, odepth), BF16), vm((rows, odepth), F32),
        vm((2, chips, rows, odepth), BF16), vm((2, chips, rows, ocols), F32),
        vm((n_tp, n_dp * seqs, ocols), F32), vm((n_tp, n_dp * seqs, ocols), BF16),
        vm((n_tp, n_dp * seqs, ocols), BF16),
        vm((n_dp, seqs, ocols), BF16), vm((n_dp, seqs, ocols), BF16),
        vm((n_tp, 2, seqs, owide), BF16), vm((n_tp, 2, seqs, owide), BF16),
        vm((8, hd), F32), vm((n_tp, 8, hd), F32), vm((seqs, width), F32),
        dma((5,)), dma((n_dp,)), dma((n_dp,)), dma, dma, dma((chips,)), dma((chips,)),
        dma((n_tp,)), dma((n_tp,)), dma((n_tp,)), dma((n_tp,)),
        dma((chips,)), dma((2, chips)), dma((chips,)), dma((n_tp,)), dma((n_tp,)),
        dma((n_dp,)), dma((n_dp,)), dma((n_tp,)), dma((n_tp,)), dma((n_tp,)), dma((n_tp,)),
    ]
    anywhere = pl.BlockSpec(memory_space=pl.ANY)
    in_vmem = pl.BlockSpec(memory_space=pltpu.VMEM)
    resid, scaled, scale = pl.pallas_call(
        functools.partial(layer, n_dp, n_tp),
        out_shape=(
            jax.ShapeDtypeStruct((rows, owide), BF16),
            jax.ShapeDtypeStruct((rows, owide), BF16),
            jax.ShapeDtypeStruct((8, hd), F32),
        ),
        in_specs=[anywhere, anywhere, anywhere, in_vmem, anywhere, pl.BlockSpec(memory_space=pltpu.SMEM)],
        out_specs=(in_vmem, in_vmem, in_vmem),
        scratch_shapes=scratch,
        compiler_params=pltpu.CompilerParams(
            collective_id=0, has_side_effects=True, vmem_limit_bytes=66_000_000),
    )(hidden, w_qkv, w_out, norm_gain.reshape(1, width), kv_cache, lengths)
    return resid, scaled, scale[0, :rows]


def solution(mesh):
    placed = (
        P("dp", None),
        P("dp", "tp"),
        P("tp", "dp"),
        P(),
        P(("dp", "tp"), None, None, None),
        P(("dp", "tp")),
    )
    n_dp, n_tp = mesh.shape["dp"], mesh.shape["tp"]

    def body(hidden, w_qkv, w_out, norm_gain, kv_cache, lengths):
        lanes = kv_cache.shape[3] // 2
        fits = (
            n_dp % 2 == 0
            and kv_cache.shape[2] == lanes
            and w_qkv.shape[1] % lanes == 0
            and w_out.shape[0] % lanes == 0
            and w_out.shape[1] % lanes == 0
            and hidden.shape[0] <= lanes
            and hidden.shape[1] // n_tp == w_out.shape[0]
        )
        if fits:
            return fused(n_dp, n_tp, hidden, w_qkv, w_out, norm_gain, kv_cache, lengths)
        return shards(hidden, w_qkv, w_out, norm_gain, kv_cache, lengths)

    return jax.shard_map(
        body,
        mesh=mesh,
        in_specs=placed,
        out_specs=(P("dp", "tp"), P("dp", "tp"), P("dp")),
        check_vma=False,
    )
```

```python
import functools

import jax
import jax.numpy as jnp
from jax import lax
from jax.experimental import pallas as pl
from jax.experimental.pallas import tpu as pltpu
from jax.sharding import PartitionSpec as P


def rope(values, positions):
    half = values.shape[-1] // 2
    freqs = 1000000.0 ** (-2.0 * jnp.arange(half, dtype=jnp.float32) / values.shape[-1])
    angle = positions[..., None] * freqs
    cosine = jnp.cos(angle)
    sine = jnp.sin(angle)
    first = values[..., :half]
    second = values[..., half:]
    return jnp.concatenate(
        [first * cosine - second * sine, second * cosine + first * sine], axis=-1
    )


def shards(hidden, w_qkv, w_out, norm_gain, kv_cache, lengths):
    seq_dev = kv_cache.shape[0]
    kv_heads = kv_cache.shape[1]
    head_size = kv_cache.shape[3] // 2
    tp_count = lax.axis_size("tp")
    w_cols = lax.all_gather(w_qkv, "dp", axis=0, tiled=True)
    qkv_part = jnp.dot(hidden, w_cols, preferred_element_type=jnp.float32)
    mine = lax.all_to_all(
        qkv_part.astype(jnp.bfloat16), "tp", split_axis=0, concat_axis=1, tiled=True
    )
    att_width = w_out.shape[0] * tp_count
    heads = att_width // head_size
    groups = heads // kv_heads
    positions = lengths.astype(jnp.float32)[:, None]
    query = rope(
        mine[:, :att_width].reshape(seq_dev, heads, head_size).astype(jnp.float32), positions
    ).astype(jnp.bfloat16)
    key_new = rope(
        mine[:, att_width : att_width + kv_heads * head_size]
        .reshape(seq_dev, kv_heads, head_size)
        .astype(jnp.float32),
        positions,
    ).astype(jnp.bfloat16)
    value_new = mine[:, att_width + kv_heads * head_size :].reshape(seq_dev, kv_heads, head_size)
    q_grp = query.reshape(seq_dev, kv_heads, groups, head_size)
    keys = kv_cache[..., :head_size]
    vals = kv_cache[..., head_size:]
    scale = 1.0 / head_size**0.5
    scores = jnp.einsum("nkgd,nkpd->nkgp", q_grp, keys, preferred_element_type=jnp.float32) * scale
    own = jnp.einsum("nkgd,nkd->nkg", q_grp, key_new, preferred_element_type=jnp.float32) * scale
    valid = (jnp.arange(kv_cache.shape[2])[None, :] < lengths[:, None])[:, None, None, :]
    scores = jnp.where(valid, scores, jnp.float32(-1e30))
    top = jnp.maximum(jnp.max(scores, axis=-1), own)
    probs = jnp.where(valid, jnp.exp(scores - top[..., None]), jnp.float32(0.0))
    own_prob = jnp.exp(own - top)
    denom = jnp.sum(probs, axis=-1) + own_prob
    weights = (probs / denom[..., None]).astype(jnp.bfloat16)
    own_weight = (own_prob / denom).astype(jnp.bfloat16)
    mixed = jnp.einsum("nkgp,nkpd->nkgd", weights, vals, preferred_element_type=jnp.float32)
    mixed = (
        mixed
        + own_weight.astype(jnp.float32)[..., None] * value_new.astype(jnp.float32)[:, :, None, :]
    )
    attn = mixed.reshape(seq_dev, att_width).astype(jnp.bfloat16)
    heads_part = lax.all_to_all(attn, "tp", split_axis=1, concat_axis=0, tiled=True)
    terms = jnp.dot(
        heads_part,
        lax.all_gather(w_out, "dp", axis=1, tiled=True),
        preferred_element_type=jnp.float32,
    )
    width = terms.shape[1]
    share = width // tp_count
    offset = lax.axis_index("tp") * share
    summed = lax.psum_scatter(
        terms.astype(jnp.bfloat16), "tp", scatter_dimension=1, tiled=True
    ).astype(jnp.float32)
    hidden_mine = lax.dynamic_slice_in_dim(hidden, offset, share, 1).astype(jnp.float32)
    gain_mine = lax.dynamic_slice_in_dim(norm_gain, offset, share, 0)
    resid_mine = hidden_mine + summed
    weighted = resid_mine * gain_mine[None, :]
    squares = lax.psum(jnp.sum(resid_mine * resid_mine, axis=-1), "tp")
    peak = lax.pmax(jnp.max(jnp.abs(weighted), axis=-1), "tp")
    inverse = lax.rsqrt(squares / width + 1e-06)
    normed_mine = weighted * inverse[:, None]
    row_scale = (peak * inverse + 1e-06) / 448.0
    residual_out = resid_mine.astype(jnp.bfloat16)
    scaled = (normed_mine / row_scale[:, None]).astype(jnp.bfloat16)
    return (residual_out, scaled, row_scale)


F32 = jnp.float32
BF16 = jnp.bfloat16
MESH = pl.DeviceIdType.MESH


def send(src, dst, send_sem, recv_sem, where):
    copy = pltpu.make_async_remote_copy(
        src_ref=src, dst_ref=dst, send_sem=send_sem, recv_sem=recv_sem,
        device_id=where, device_id_type=MESH,
    )
    copy.start()
    return copy


def layer(
    n_dp, n_tp,
    hidden, w_qkv, w_out, gain, cache, lens,
    resid_out, scaled_out, scale_out,
    h_all, w1, w2, kv, hid, hid32, p_send, p_recv, r_acc, r_send, r_recv,
    q_rows, k_rows, v_rows, l_rows, s_rows, a_rows,
    t2_send, t2_recv, b_rows, ag, mm, f_send, f_recv,
    o_send, o_recv, c_send, c_recv, fin,
    loc_sem, h_s, h_r, p_s, p_r, r_s, r_r, t2_s, t2_r,
    g_s, g_r, x_s, f_s, f_r, o_s, o_r, c_s, c_r,
):
    dp = lax.axis_index("dp")
    tp = lax.axis_index("tp")
    core = lax.rem(dp, 2)
    chip = dp // 2
    other = 1 - core
    partner = chip * 2 + other
    n_chip = n_dp // 2
    rows = hidden.shape[0]
    seqs = rows // n_tp
    depth = w_qkv.shape[0]
    ocols = w_out.shape[1]
    owide = resid_out.shape[1]
    kvh = cache.shape[1]
    ctx = cache.shape[2]
    hd = cache.shape[3] // 2
    heads = (w_out.shape[0] * n_tp) // hd
    groups = heads // kvh
    per = w_qkv.shape[1] // hd
    per_out = w_out.shape[0] // hd
    width = hidden.shape[1]

    own_h = pltpu.make_async_copy(
        hidden.at[:, pl.ds(pl.multiple_of(dp * depth, depth), depth)], h_all.at[core, chip], loc_sem.at[0])
    own_h.start()
    load_w1 = pltpu.make_async_copy(w_qkv, w1, loc_sem.at[1])
    load_w1.start()

    barrier = pltpu.get_barrier_semaphore()
    for d in range(n_dp):
        for e in range(n_tp):
            if d or e:
                pl.semaphore_signal(
                    barrier, inc=1, device_id_type=MESH,
                    device_id={"dp": lax.rem(dp + d, n_dp), "tp": lax.rem(tp + e, n_tp)})
    pl.semaphore_wait(barrier, n_dp * n_tp - 1)

    pending = []
    for d in range(1, n_dp):
        peer = lax.rem(dp + d, n_dp)
        pending.append(send(
            hidden.at[:, pl.ds(pl.multiple_of(peer * depth, depth), depth)],
            h_all.at[core, chip], h_s.at[peer], h_r.at[dp], {"dp": peer}))
    load_kv = pltpu.make_async_copy(cache, kv, loc_sem.at[2])
    load_kv.start()
    load_w2 = pltpu.make_async_copy(w_out, w2, loc_sem.at[3])
    load_w2.start()
    load_hid = pltpu.make_async_copy(hidden, hid, loc_sem.at[4])
    load_hid.start()

    row_i = lax.broadcasted_iota(jnp.int32, (seqs, hd), 0)
    lane_i = lax.broadcasted_iota(jnp.int32, (seqs, hd), 1)
    live = jnp.zeros((seqs, hd), jnp.int32)
    for n in range(seqs):
        live = jnp.where(row_i == n, lens[n], live)
    half = hd // 2
    low = lane_i < half
    index = jnp.where(low, lane_i, lane_i - half).astype(F32)
    freqs = jnp.exp(index * F32(-2.0 * 13.815510557964274 / hd))
    angle = live.astype(F32) * freqs
    cosine = jnp.cos(angle)
    sine = jnp.where(low, -jnp.sin(angle), jnp.sin(angle))
    for h in range(heads):
        l_rows[pl.ds(h, seqs, stride=heads), :] = live.astype(F32)
    load_hid.wait()
    hid32[...] = hid[...].astype(F32)

    def recv_h(peer):
        pltpu.make_async_remote_copy(
            src_ref=h_all.at[core, chip], dst_ref=h_all.at[lax.rem(peer, 2), peer // 2],
            send_sem=h_s.at[peer], recv_sem=h_r.at[peer],
            device_id={"dp": peer}, device_id_type=MESH).wait_recv()

    own_h.wait()
    load_w1.wait()
    for d in range(n_chip):
        recv_h(2 * d + other)
    part = jnp.dot(h_all[other].reshape(n_chip * rows, depth), w1[...], preferred_element_type=F32)
    p_send[...] = part.astype(BF16).reshape(p_send.shape)
    swap = send(p_send, p_recv, p_s, p_r, {"dp": partner})
    pending.append(swap)
    for d in range(1, n_chip):
        recv_h(2 * lax.rem(chip + d, n_chip) + core)
    part = jnp.dot(h_all[core].reshape(n_chip * rows, depth), w1[...], preferred_element_type=F32)
    r_acc[...] = part.reshape(r_acc.shape)
    swap.wait_recv()
    order = sorted(range(n_chip), key=lambda d: -min(d, n_chip - d))
    for d in order:
        to = lax.rem(chip + d, n_chip)
        r_acc[to] = r_acc[to] + p_recv[to].astype(F32)
        for q in range(n_tp):
            r_send[to, q] = r_acc[to, q * seqs : (q + 1) * seqs, :].astype(BF16)
        for e in reversed(range(n_tp)):
            peer = lax.rem(tp + e, n_tp)
            if d or e:
                pending.append(send(
                    r_send.at[to, peer], r_recv.at[chip, tp], r_s.at[to, peer], r_r.at[chip, tp],
                    {"dp": to * 2 + core, "tp": peer}))
            else:
                keep = pltpu.make_async_copy(r_send.at[chip, tp], r_recv.at[chip, tp], loc_sem.at[0])
                keep.start()
    keep.wait()
    for d in reversed(order):
        who = lax.rem(chip + d, n_chip)
        for e in range(n_tp):
            peer = lax.rem(tp + e, n_tp)
            if d or e:
                pltpu.make_async_remote_copy(
                    src_ref=r_send.at[who, peer], dst_ref=r_recv.at[who, peer],
                    send_sem=r_s.at[who, peer], recv_sem=r_r.at[who, peer],
                    device_id={"dp": who * 2 + core, "tp": peer}, device_id_type=MESH).wait_recv()

    def exchange(src, dst, s_sem, r_sem, fill):
        for q in range(n_tp):
            fill(q)
        keep = pltpu.make_async_copy(src.at[tp], dst.at[tp], r_sem.at[tp])
        keep.start()
        sent = []
        for d in range(1, n_tp):
            peer = lax.rem(tp + d, n_tp)
            sent.append(send(src.at[peer], dst.at[tp], s_sem.at[peer], r_sem.at[tp], {"tp": peer}))
        keep.wait()
        for d in range(1, n_tp):
            peer = lax.rem(tp + d, n_tp)
            pltpu.make_async_remote_copy(
                src_ref=src.at[peer], dst_ref=dst.at[peer], send_sem=s_sem.at[peer], recv_sem=r_sem.at[peer],
                device_id={"tp": peer}, device_id_type=MESH).wait_recv()
        return sent

    def head(h):
        at = slice((h % per) * hd, (h % per + 1) * hd)
        total = r_recv[0, h // per, :, at].astype(F32)
        for c in range(1, n_chip):
            total = total + r_recv[c, h // per, :, at].astype(F32)
        return total.astype(BF16).astype(F32)

    def turn(x):
        return (x * cosine + pltpu.roll(x, half, 1) * sine).astype(BF16).astype(F32)

    for h in range(heads):
        q_rows[pl.ds(h, seqs, stride=heads), :] = turn(head(h))
    for k in range(kvh):
        key_new = turn(head(heads + k))
        value_new = head(heads + kvh + k)
        for g in range(groups):
            k_rows[pl.ds(k * groups + g, seqs, stride=heads), :] = key_new
            v_rows[pl.ds(k * groups + g, seqs, stride=heads), :] = value_new
    load_kv.wait()
    for n in range(seqs):
        for k in range(kvh):
            at = (n * kvh + k) * groups
            s_rows[at : at + groups, :] = lax.dot_general(
                q_rows[at : at + groups, :].astype(BF16), kv[n, k, :, :hd],
                (((1,), (1,)), ((), ())), preferred_element_type=F32)
    factor = F32(1.0 / hd**0.5)
    pos = lax.broadcasted_iota(jnp.int32, (seqs * heads, ctx), 1).astype(F32)
    valid = pos < l_rows[...]
    scores = jnp.where(valid, s_rows[...] * factor, F32(-1e30))
    own = jnp.sum(q_rows[...] * k_rows[...], axis=1, keepdims=True) * factor
    top = jnp.maximum(jnp.max(scores, axis=1, keepdims=True), own)
    probs = jnp.where(valid, jnp.exp(scores - top), F32(0.0))
    own_prob = jnp.exp(own - top)
    denom = jnp.sum(probs, axis=1, keepdims=True) + own_prob
    s_rows[...] = probs / denom
    own_weight = (own_prob / denom).astype(BF16).astype(F32)
    v_rows[...] = own_weight * v_rows[...]
    for n in range(seqs):
        for k in range(kvh):
            at = (n * kvh + k) * groups
            a_rows[at : at + groups, :] = jnp.dot(
                s_rows[at : at + groups, :].astype(BF16), kv[n, k, :, hd:],
                preferred_element_type=F32) + v_rows[at : at + groups, :]

    def fill2(q):
        for e in range(per_out):
            t2_send[q, :, e * hd : (e + 1) * hd] = a_rows[
                pl.ds(q * per_out + e, seqs, stride=heads), :].astype(BF16)

    pending += exchange(t2_send, t2_recv, t2_s, t2_r, fill2)
    for q in range(n_tp):
        b_rows[q * seqs : (q + 1) * seqs, :] = t2_recv[q].astype(F32)
    ag[core, chip] = b_rows[...].astype(BF16)
    for d in range(1, n_chip):
        to = lax.rem(chip + d, n_chip)
        pending.append(send(ag.at[core, chip], ag.at[core, chip], g_s.at[to], g_r.at[core, chip],
                            {"dp": to * 2 + core}))
    pending.append(send(ag.at[core, chip], ag.at[core, chip], x_s.at[chip], g_r.at[core, chip], {"dp": partner}))

    def recv_g(c, who):
        pltpu.make_async_remote_copy(
            src_ref=ag.at[core, chip], dst_ref=ag.at[c, who], send_sem=x_s.at[chip], recv_sem=g_r.at[c, who],
            device_id={"dp": partner}, device_id_type=MESH).wait_recv()

    for d in range(1, n_chip):
        who = lax.rem(chip + d, n_chip)
        recv_g(core, who)
        pending.append(send(ag.at[core, who], ag.at[core, who], x_s.at[who], g_r.at[core, who], {"dp": partner}))
    load_w2.wait()
    def project(side):
        mm[side] = jnp.dot(ag[side].reshape(n_chip * rows, w_out.shape[0]), w2[...],
                           preferred_element_type=F32).reshape(n_chip, rows, ocols)
        for d in order:
            to = lax.rem(chip + d, n_chip)
            for q in range(n_tp):
                f_send[side, to, q] = mm[side, to, q * seqs : (q + 1) * seqs, :].astype(BF16)
            for e in reversed(range(n_tp)):
                peer = lax.rem(tp + e, n_tp)
                if d or e or side is not core:
                    pending.append(send(
                        f_send.at[side, to, peer], f_recv.at[tp, dp], f_s.at[side, to, peer], f_r.at[tp, dp],
                        {"dp": to * 2 + side, "tp": peer}))
                else:
                    pltpu.make_async_copy(f_send.at[side, to, peer], f_recv.at[tp, dp], loc_sem.at[0]).start()

    project(core)
    for d in range(n_chip):
        recv_g(other, d)
    project(other)
    pltpu.make_async_copy(f_send.at[core, chip, tp], f_recv.at[tp, dp], loc_sem.at[0]).wait()
    for d in range(n_dp):
        who = lax.rem(dp + d, n_dp)
        for e in range(n_tp):
            peer = lax.rem(tp + e, n_tp)
            if d or e:
                pltpu.make_async_remote_copy(
                    src_ref=f_send.at[core, chip, peer], dst_ref=f_recv.at[peer, who],
                    send_sem=f_s.at[core, chip, peer], recv_sem=f_r.at[peer, who],
                    device_id={"dp": who, "tp": peer}, device_id_type=MESH).wait_recv()
    for r in range(n_dp):
        block = slice(r * ocols, (r + 1) * ocols)
        mine = hid32[0:seqs, block]
        for q in range(1, n_tp):
            mine = jnp.where(tp == q, hid32[q * seqs : (q + 1) * seqs, block], mine)
        total = f_recv[0, r].astype(F32)
        for q in range(1, n_tp):
            total = total + f_recv[q, r].astype(F32)
        fin[:, block] = mine + total
    resid = fin[...]
    inverse = lax.rsqrt(jnp.sum(resid * resid, axis=1, keepdims=True) / width + F32(1e-06))
    weighted = resid * gain[...]
    peak = jnp.max(jnp.abs(weighted), axis=1, keepdims=True)
    scale = (peak * inverse + F32(1e-06)) / F32(448.0)
    scaled = (weighted * (inverse / scale)).astype(BF16)
    for q in range(n_tp):
        o_send[q, 0] = resid[:, q * owide : (q + 1) * owide].astype(BF16)
        o_send[q, 1] = scaled[:, q * owide : (q + 1) * owide]
    spread = jnp.where(lane_i == row_i + tp * seqs, jnp.broadcast_to(scale, lane_i.shape), F32(0.0))
    c_send[...] = jnp.broadcast_to(jnp.sum(spread, axis=0, keepdims=True), c_send.shape)
    for d in range(1, n_tp):
        peer = lax.rem(tp + d, n_tp)
        pending.append(send(c_send, c_recv.at[tp], c_s.at[peer], c_r.at[tp], {"tp": peer}))
    pending += exchange(o_send, o_recv, o_s, o_r, lambda q: None)
    scales = c_send[...]
    for d in range(1, n_tp):
        peer = lax.rem(tp + d, n_tp)
        pltpu.make_async_remote_copy(
            src_ref=c_send, dst_ref=c_recv.at[peer], send_sem=c_s.at[peer], recv_sem=c_r.at[peer],
            device_id={"tp": peer}, device_id_type=MESH).wait_recv()
        scales = scales + c_recv[peer]
    scale_out[...] = scales
    for part, out in ((0, resid_out), (1, scaled_out)):
        for q in range(n_tp):
            b_rows[q * seqs : (q + 1) * seqs, :] = o_recv[q, part].astype(F32)
        out[...] = b_rows[...].astype(BF16)
    for copy in pending:
        copy.wait_send()


def finish(resid, scaled, scale, resid_out, scaled_out, scale_out):
    resid_out[...] = resid[...]
    scaled_out[...] = scaled[...]
    scale_out[...] = scale[0:1, : scale_out.shape[1]]


def fused(n_dp, n_tp, hidden, w_qkv, w_out, norm_gain, kv_cache, lengths):
    rows, width = hidden.shape
    seqs, kvh, ctx, hd2 = kv_cache.shape
    hd = hd2 // 2
    depth, cols = w_qkv.shape
    odepth, ocols = w_out.shape
    heads = odepth * n_tp // hd
    owide = width // n_tp
    chips = n_dp // 2
    vm = pltpu.VMEM
    dma = pltpu.SemaphoreType.DMA
    all_rows = seqs * heads
    scratch = [
        vm((2, chips, rows, depth), BF16), vm((depth, cols), BF16), vm((odepth, ocols), BF16),
        vm(kv_cache.shape, BF16), vm((rows, width), BF16), vm((rows, width), F32),
        vm((chips, rows, cols), BF16), vm((chips, rows, cols), BF16), vm((chips, rows, cols), F32),
        vm((chips, n_tp, seqs, cols), BF16), vm((chips, n_tp, seqs, cols), BF16),
        vm((all_rows, hd), F32), vm((all_rows, hd), F32), vm((all_rows, hd), F32), vm((all_rows, hd), F32),
        vm((all_rows, ctx), F32), vm((all_rows, hd), F32),
        vm((n_tp, seqs, odepth), BF16), vm((n_tp, seqs, odepth), BF16), vm((rows, odepth), F32),
        vm((2, chips, rows, odepth), BF16), vm((2, chips, rows, ocols), F32),
        vm((2, chips, n_tp, seqs, ocols), BF16), vm((n_tp, n_dp, seqs, ocols), BF16),
        vm((n_tp, 2, seqs, owide), BF16), vm((n_tp, 2, seqs, owide), BF16),
        vm((8, hd), F32), vm((n_tp, 8, hd), F32), vm((seqs, width), F32),
        dma((5,)), dma((n_dp,)), dma((n_dp,)), dma, dma, dma((chips, n_tp)), dma((chips, n_tp)),
        dma((n_tp,)), dma((n_tp,)),
        dma((chips,)), dma((2, chips)), dma((chips,)),
        dma((2, chips, n_tp)), dma((n_tp, n_dp)), dma((n_tp,)), dma((n_tp,)), dma((n_tp,)), dma((n_tp,)),
    ]
    anywhere = pl.BlockSpec(memory_space=pl.ANY)
    in_vmem = pl.BlockSpec(memory_space=pltpu.VMEM)
    resid, scaled, scale = pl.pallas_call(
        functools.partial(layer, n_dp, n_tp),
        out_shape=(
            jax.ShapeDtypeStruct((rows, owide), BF16),
            jax.ShapeDtypeStruct((rows, owide), BF16),
            jax.ShapeDtypeStruct((8, hd), F32),
        ),
        in_specs=[anywhere, anywhere, anywhere, in_vmem, anywhere, pl.BlockSpec(memory_space=pltpu.SMEM)],
        out_specs=(in_vmem, in_vmem, in_vmem),
        scratch_shapes=scratch,
        compiler_params=pltpu.CompilerParams(
            collective_id=0, has_side_effects=True, vmem_limit_bytes=66_000_000),
    )(hidden, w_qkv, w_out, norm_gain.reshape(1, width), kv_cache, lengths)
    resid, scaled, scale = pl.pallas_call(
        finish,
        out_shape=(
            jax.ShapeDtypeStruct((rows, owide), BF16),
            jax.ShapeDtypeStruct((rows, owide), BF16),
            jax.ShapeDtypeStruct((1, rows), F32),
        ),
        in_specs=[in_vmem, in_vmem, in_vmem],
        out_specs=(in_vmem, in_vmem, in_vmem),
    )(resid, scaled, scale)
    return resid, scaled, scale.reshape(rows)


def solution(mesh):
    placed = (
        P("dp", None),
        P("dp", "tp"),
        P("tp", "dp"),
        P(),
        P(("dp", "tp"), None, None, None),
        P(("dp", "tp")),
    )
    n_dp, n_tp = mesh.shape["dp"], mesh.shape["tp"]

    def body(hidden, w_qkv, w_out, norm_gain, kv_cache, lengths):
        lanes = kv_cache.shape[3] // 2
        fits = (
            n_dp % 2 == 0
            and kv_cache.shape[2] == lanes
            and w_qkv.shape[1] % lanes == 0
            and w_out.shape[0] % lanes == 0
            and w_out.shape[1] % lanes == 0
            and hidden.shape[0] <= lanes
            and hidden.shape[1] // n_tp == w_out.shape[0]
        )
        if fits:
            return fused(n_dp, n_tp, hidden, w_qkv, w_out, norm_gain, kv_cache, lengths)
        return shards(hidden, w_qkv, w_out, norm_gain, kv_cache, lengths)

    return jax.shard_map(
        body,
        mesh=mesh,
        in_specs=placed,
        out_specs=(P("dp", "tp"), P("dp", "tp"), P("dp")),
        check_vma=False,
    )
```

```python
import functools

import jax
import jax.numpy as jnp
from jax import lax
from jax.experimental import pallas as pl
from jax.experimental.pallas import tpu as pltpu
from jax.sharding import PartitionSpec as P


def rope(values, positions):
    half = values.shape[-1] // 2
    freqs = 1000000.0 ** (-2.0 * jnp.arange(half, dtype=jnp.float32) / values.shape[-1])
    angle = positions[..., None] * freqs
    cosine = jnp.cos(angle)
    sine = jnp.sin(angle)
    first = values[..., :half]
    second = values[..., half:]
    return jnp.concatenate(
        [first * cosine - second * sine, second * cosine + first * sine], axis=-1
    )


def shards(hidden, w_qkv, w_out, norm_gain, kv_cache, lengths):
    seq_dev = kv_cache.shape[0]
    kv_heads = kv_cache.shape[1]
    head_size = kv_cache.shape[3] // 2
    tp_count = lax.axis_size("tp")
    w_cols = lax.all_gather(w_qkv, "dp", axis=0, tiled=True)
    qkv_part = jnp.dot(hidden, w_cols, preferred_element_type=jnp.float32)
    mine = lax.all_to_all(
        qkv_part.astype(jnp.bfloat16), "tp", split_axis=0, concat_axis=1, tiled=True
    )
    att_width = w_out.shape[0] * tp_count
    heads = att_width // head_size
    groups = heads // kv_heads
    positions = lengths.astype(jnp.float32)[:, None]
    query = rope(
        mine[:, :att_width].reshape(seq_dev, heads, head_size).astype(jnp.float32), positions
    ).astype(jnp.bfloat16)
    key_new = rope(
        mine[:, att_width : att_width + kv_heads * head_size]
        .reshape(seq_dev, kv_heads, head_size)
        .astype(jnp.float32),
        positions,
    ).astype(jnp.bfloat16)
    value_new = mine[:, att_width + kv_heads * head_size :].reshape(seq_dev, kv_heads, head_size)
    q_grp = query.reshape(seq_dev, kv_heads, groups, head_size)
    keys = kv_cache[..., :head_size]
    vals = kv_cache[..., head_size:]
    scale = 1.0 / head_size**0.5
    scores = jnp.einsum("nkgd,nkpd->nkgp", q_grp, keys, preferred_element_type=jnp.float32) * scale
    own = jnp.einsum("nkgd,nkd->nkg", q_grp, key_new, preferred_element_type=jnp.float32) * scale
    valid = (jnp.arange(kv_cache.shape[2])[None, :] < lengths[:, None])[:, None, None, :]
    scores = jnp.where(valid, scores, jnp.float32(-1e30))
    top = jnp.maximum(jnp.max(scores, axis=-1), own)
    probs = jnp.where(valid, jnp.exp(scores - top[..., None]), jnp.float32(0.0))
    own_prob = jnp.exp(own - top)
    denom = jnp.sum(probs, axis=-1) + own_prob
    weights = (probs / denom[..., None]).astype(jnp.bfloat16)
    own_weight = (own_prob / denom).astype(jnp.bfloat16)
    mixed = jnp.einsum("nkgp,nkpd->nkgd", weights, vals, preferred_element_type=jnp.float32)
    mixed = (
        mixed
        + own_weight.astype(jnp.float32)[..., None] * value_new.astype(jnp.float32)[:, :, None, :]
    )
    attn = mixed.reshape(seq_dev, att_width).astype(jnp.bfloat16)
    heads_part = lax.all_to_all(attn, "tp", split_axis=1, concat_axis=0, tiled=True)
    terms = jnp.dot(
        heads_part,
        lax.all_gather(w_out, "dp", axis=1, tiled=True),
        preferred_element_type=jnp.float32,
    )
    width = terms.shape[1]
    share = width // tp_count
    offset = lax.axis_index("tp") * share
    summed = lax.psum_scatter(
        terms.astype(jnp.bfloat16), "tp", scatter_dimension=1, tiled=True
    ).astype(jnp.float32)
    hidden_mine = lax.dynamic_slice_in_dim(hidden, offset, share, 1).astype(jnp.float32)
    gain_mine = lax.dynamic_slice_in_dim(norm_gain, offset, share, 0)
    resid_mine = hidden_mine + summed
    weighted = resid_mine * gain_mine[None, :]
    squares = lax.psum(jnp.sum(resid_mine * resid_mine, axis=-1), "tp")
    peak = lax.pmax(jnp.max(jnp.abs(weighted), axis=-1), "tp")
    inverse = lax.rsqrt(squares / width + 1e-06)
    normed_mine = weighted * inverse[:, None]
    row_scale = (peak * inverse + 1e-06) / 448.0
    residual_out = resid_mine.astype(jnp.bfloat16)
    scaled = (normed_mine / row_scale[:, None]).astype(jnp.bfloat16)
    return (residual_out, scaled, row_scale)


F32 = jnp.float32
BF16 = jnp.bfloat16
MESH = pl.DeviceIdType.MESH


def send(src, dst, send_sem, recv_sem, where):
    copy = pltpu.make_async_remote_copy(
        src_ref=src, dst_ref=dst, send_sem=send_sem, recv_sem=recv_sem,
        device_id=where, device_id_type=MESH,
    )
    copy.start()
    return copy


def layer(
    n_dp, n_tp,
    hidden, w_qkv, w_out, gain, cache, lens,
    resid_out, scaled_out, scale_out,
    h_all, w1, w2, kv, hid, hid32, p_send, p_recv, r_acc, r_send, r_recv, mine32,
    t1_send, t1_recv, q_rows, k_rows, v_rows, l_rows, s_rows, a_rows,
    t2_send, t2_recv, b_rows, ag, mm, mq, t3_send, t3_recv, f_send, f_recv,
    o_send, o_recv, c_send, c_recv, fin,
    loc_sem, h_s, h_r, p_s, p_r, r_s, r_r, t1_s, t1_r, t2_s, t2_r,
    g_s, g_r, x_s, t3_s, t3_r, f_s, f_r, o_s, o_r, c_s, c_r,
):
    dp = lax.axis_index("dp")
    tp = lax.axis_index("tp")
    core = lax.rem(dp, 2)
    chip = dp // 2
    other = 1 - core
    partner = chip * 2 + other
    n_chip = n_dp // 2
    rows = hidden.shape[0]
    seqs = rows // n_tp
    depth = w_qkv.shape[0]
    ocols = w_out.shape[1]
    owide = resid_out.shape[1]
    kvh = cache.shape[1]
    ctx = cache.shape[2]
    hd = cache.shape[3] // 2
    heads = (w_out.shape[0] * n_tp) // hd
    groups = heads // kvh
    per = w_qkv.shape[1] // hd
    per_out = w_out.shape[0] // hd
    width = hidden.shape[1]

    own_h = pltpu.make_async_copy(
        hidden.at[:, pl.ds(pl.multiple_of(dp * depth, depth), depth)], h_all.at[core, chip], loc_sem.at[0])
    own_h.start()
    load_w1 = pltpu.make_async_copy(w_qkv, w1, loc_sem.at[1])
    load_w1.start()

    barrier = pltpu.get_barrier_semaphore()
    for d in range(1, n_dp):
        pl.semaphore_signal(barrier, inc=1, device_id={"dp": lax.rem(dp + d, n_dp)}, device_id_type=MESH)
    for d in range(1, n_tp):
        pl.semaphore_signal(barrier, inc=1, device_id={"tp": lax.rem(tp + d, n_tp)}, device_id_type=MESH)
    pl.semaphore_wait(barrier, n_dp + n_tp - 2)

    pending = []
    for d in range(1, n_dp):
        peer = lax.rem(dp + d, n_dp)
        pending.append(send(
            hidden.at[:, pl.ds(pl.multiple_of(peer * depth, depth), depth)],
            h_all.at[core, chip], h_s.at[peer], h_r.at[dp], {"dp": peer}))
    load_kv = pltpu.make_async_copy(cache, kv, loc_sem.at[2])
    load_kv.start()
    load_w2 = pltpu.make_async_copy(w_out, w2, loc_sem.at[3])
    load_w2.start()
    load_hid = pltpu.make_async_copy(hidden, hid, loc_sem.at[4])
    load_hid.start()

    row_i = lax.broadcasted_iota(jnp.int32, (seqs, hd), 0)
    lane_i = lax.broadcasted_iota(jnp.int32, (seqs, hd), 1)
    live = jnp.zeros((seqs, hd), jnp.int32)
    for n in range(seqs):
        live = jnp.where(row_i == n, lens[n], live)
    half = hd // 2
    low = lane_i < half
    index = jnp.where(low, lane_i, lane_i - half).astype(F32)
    freqs = jnp.exp(index * F32(-2.0 * 13.815510557964274 / hd))
    angle = live.astype(F32) * freqs
    cosine = jnp.cos(angle)
    sine = jnp.where(low, -jnp.sin(angle), jnp.sin(angle))
    for h in range(heads):
        l_rows[pl.ds(h, seqs, stride=heads), :] = live.astype(F32)
    load_hid.wait()
    hid32[...] = hid[...].astype(F32)

    def recv_h(peer):
        pltpu.make_async_remote_copy(
            src_ref=h_all.at[core, chip], dst_ref=h_all.at[lax.rem(peer, 2), peer // 2],
            send_sem=h_s.at[peer], recv_sem=h_r.at[peer],
            device_id={"dp": peer}, device_id_type=MESH).wait_recv()

    own_h.wait()
    load_w1.wait()
    for d in range(n_chip):
        recv_h(2 * d + other)
    part = jnp.dot(h_all[other].reshape(n_chip * rows, depth), w1[...], preferred_element_type=F32)
    p_send[...] = part.astype(BF16).reshape(p_send.shape)
    swap = send(p_send, p_recv, p_s, p_r, {"dp": partner})
    pending.append(swap)
    for d in range(1, n_chip):
        recv_h(2 * lax.rem(chip + d, n_chip) + core)
    part = jnp.dot(h_all[core].reshape(n_chip * rows, depth), w1[...], preferred_element_type=F32)
    r_acc[...] = part.reshape(r_acc.shape)
    swap.wait_recv()
    for d in range(1, n_chip):
        to = lax.rem(chip + d, n_chip)
        r_send[to] = (r_acc[to] + p_recv[to].astype(F32)).astype(BF16)
        pending.append(send(r_send.at[to], r_recv.at[chip], r_s.at[to], r_r.at[chip], {"dp": to * 2 + core}))
    total = r_acc[chip] + p_recv[chip].astype(F32)
    for d in range(1, n_chip):
        who = lax.rem(chip + d, n_chip)
        pltpu.make_async_remote_copy(
            src_ref=r_send.at[who], dst_ref=r_recv.at[who], send_sem=r_s.at[who], recv_sem=r_r.at[who],
            device_id={"dp": who * 2 + core}, device_id_type=MESH).wait_recv()
        total = total + r_recv[who].astype(F32)
    mine32[...] = total

    def exchange(src, dst, s_sem, r_sem, fill):
        for q in range(n_tp):
            fill(q)
        keep = pltpu.make_async_copy(src.at[tp], dst.at[tp], r_sem.at[tp])
        keep.start()
        sent = []
        for d in range(1, n_tp):
            peer = lax.rem(tp + d, n_tp)
            sent.append(send(src.at[peer], dst.at[tp], s_sem.at[peer], r_sem.at[tp], {"tp": peer}))
        keep.wait()
        for d in range(1, n_tp):
            peer = lax.rem(tp + d, n_tp)
            pltpu.make_async_remote_copy(
                src_ref=src.at[peer], dst_ref=dst.at[peer], send_sem=s_sem.at[peer], recv_sem=r_sem.at[peer],
                device_id={"tp": peer}, device_id_type=MESH).wait_recv()
        return sent

    def fill1(q):
        t1_send[q] = mine32[q * seqs : (q + 1) * seqs, :].astype(BF16)

    pending += exchange(t1_send, t1_recv, t1_s, t1_r, fill1)

    def head(h):
        return t1_recv[h // per, :, (h % per) * hd : (h % per + 1) * hd].astype(F32)

    def turn(x):
        return (x * cosine + pltpu.roll(x, half, 1) * sine).astype(BF16).astype(F32)

    for h in range(heads):
        q_rows[pl.ds(h, seqs, stride=heads), :] = turn(head(h))
    for k in range(kvh):
        key_new = turn(head(heads + k))
        value_new = head(heads + kvh + k)
        for g in range(groups):
            k_rows[pl.ds(k * groups + g, seqs, stride=heads), :] = key_new
            v_rows[pl.ds(k * groups + g, seqs, stride=heads), :] = value_new
    load_kv.wait()
    for n in range(seqs):
        for k in range(kvh):
            at = (n * kvh + k) * groups
            s_rows[at : at + groups, :] = lax.dot_general(
                q_rows[at : at + groups, :].astype(BF16), kv[n, k, :, :hd],
                (((1,), (1,)), ((), ())), preferred_element_type=F32)
    factor = F32(1.0 / hd**0.5)
    pos = lax.broadcasted_iota(jnp.int32, (seqs * heads, ctx), 1).astype(F32)
    valid = pos < l_rows[...]
    scores = jnp.where(valid, s_rows[...] * factor, F32(-1e30))
    own = jnp.sum(q_rows[...] * k_rows[...], axis=1, keepdims=True) * factor
    top = jnp.maximum(jnp.max(scores, axis=1, keepdims=True), own)
    probs = jnp.where(valid, jnp.exp(scores - top), F32(0.0))
    own_prob = jnp.exp(own - top)
    denom = jnp.sum(probs, axis=1, keepdims=True) + own_prob
    s_rows[...] = probs / denom
    own_weight = (own_prob / denom).astype(BF16).astype(F32)
    v_rows[...] = own_weight * v_rows[...]
    for n in range(seqs):
        for k in range(kvh):
            at = (n * kvh + k) * groups
            a_rows[at : at + groups, :] = jnp.dot(
                s_rows[at : at + groups, :].astype(BF16), kv[n, k, :, hd:],
                preferred_element_type=F32) + v_rows[at : at + groups, :]

    def fill2(q):
        for e in range(per_out):
            t2_send[q, :, e * hd : (e + 1) * hd] = a_rows[
                pl.ds(q * per_out + e, seqs, stride=heads), :].astype(BF16)

    pending += exchange(t2_send, t2_recv, t2_s, t2_r, fill2)
    for q in range(n_tp):
        b_rows[q * seqs : (q + 1) * seqs, :] = t2_recv[q].astype(F32)
    ag[core, chip] = b_rows[...].astype(BF16)
    for d in range(1, n_chip):
        to = lax.rem(chip + d, n_chip)
        pending.append(send(ag.at[core, chip], ag.at[core, chip], g_s.at[to], g_r.at[core, chip],
                            {"dp": to * 2 + core}))
    pending.append(send(ag.at[core, chip], ag.at[core, chip], x_s.at[chip], g_r.at[core, chip], {"dp": partner}))

    def recv_g(c, who):
        pltpu.make_async_remote_copy(
            src_ref=ag.at[core, chip], dst_ref=ag.at[c, who], send_sem=x_s.at[chip], recv_sem=g_r.at[c, who],
            device_id={"dp": partner}, device_id_type=MESH).wait_recv()

    for d in range(1, n_chip):
        who = lax.rem(chip + d, n_chip)
        recv_g(core, who)
        pending.append(send(ag.at[core, who], ag.at[core, who], x_s.at[who], g_r.at[core, who], {"dp": partner}))
    load_w2.wait()
    def project(side):
        mm[side] = jnp.dot(ag[side].reshape(n_chip * rows, w_out.shape[0]), w2[...],
                           preferred_element_type=F32).reshape(n_chip, rows, ocols)
        for q in range(n_tp):
            for c in range(n_chip):
                mq[q, side, c * seqs : (c + 1) * seqs, :] = mm[side, c, q * seqs : (q + 1) * seqs, :]
            t3_send[q, side] = mq[q, side].astype(BF16)
        for d in range(1, n_tp):
            peer = lax.rem(tp + d, n_tp)
            pending.append(send(
                t3_send.at[peer, side], t3_recv.at[tp, side], t3_s.at[peer, side], t3_r.at[tp, side],
                {"tp": peer}))

    def scatter(side):
        total = t3_send[tp, side].astype(F32)
        for d in range(1, n_tp):
            peer = lax.rem(tp + d, n_tp)
            pltpu.make_async_remote_copy(
                src_ref=t3_send.at[peer, side], dst_ref=t3_recv.at[peer, side],
                send_sem=t3_s.at[peer, side], recv_sem=t3_r.at[peer, side],
                device_id={"tp": peer}, device_id_type=MESH).wait_recv()
            total = total + t3_recv[peer, side].astype(F32)
        mq[0, side] = total
        for c in range(n_chip):
            f_send[2 * c + side] = mq[0, side, c * seqs : (c + 1) * seqs, :].astype(BF16)
        for d in range(n_chip):
            to = 2 * lax.rem(chip + d, n_chip) + side
            if d or side is not core:
                pending.append(send(f_send.at[to], f_recv.at[dp], f_s.at[to], f_r.at[dp], {"dp": to}))
            else:
                pltpu.make_async_copy(f_send.at[dp], f_recv.at[dp], loc_sem.at[0]).start()

    project(core)
    for d in range(n_chip):
        recv_g(other, d)
    project(other)
    scatter(core)
    scatter(other)
    pltpu.make_async_copy(f_send.at[dp], f_recv.at[dp], loc_sem.at[0]).wait()
    for d in range(1, n_dp):
        peer = lax.rem(dp + d, n_dp)
        pltpu.make_async_remote_copy(
            src_ref=f_send.at[peer], dst_ref=f_recv.at[peer], send_sem=f_s.at[peer], recv_sem=f_r.at[peer],
            device_id={"dp": peer}, device_id_type=MESH).wait_recv()
    for r in range(n_dp):
        block = slice(r * ocols, (r + 1) * ocols)
        mine = hid32[0:seqs, block]
        for q in range(1, n_tp):
            mine = jnp.where(tp == q, hid32[q * seqs : (q + 1) * seqs, block], mine)
        fin[:, block] = mine + f_recv[r].astype(F32)
    resid = fin[...]
    inverse = lax.rsqrt(jnp.sum(resid * resid, axis=1, keepdims=True) / width + F32(1e-06))
    weighted = resid * gain[...]
    peak = jnp.max(jnp.abs(weighted), axis=1, keepdims=True)
    scale = (peak * inverse + F32(1e-06)) / F32(448.0)
    scaled = (weighted * (inverse / scale)).astype(BF16)
    for q in range(n_tp):
        o_send[q, 0] = resid[:, q * owide : (q + 1) * owide].astype(BF16)
        o_send[q, 1] = scaled[:, q * owide : (q + 1) * owide]
    spread = jnp.where(lane_i == row_i + tp * seqs, jnp.broadcast_to(scale, lane_i.shape), F32(0.0))
    c_send[...] = jnp.broadcast_to(jnp.sum(spread, axis=0, keepdims=True), c_send.shape)
    for d in range(1, n_tp):
        peer = lax.rem(tp + d, n_tp)
        pending.append(send(c_send, c_recv.at[tp], c_s.at[peer], c_r.at[tp], {"tp": peer}))
    pending += exchange(o_send, o_recv, o_s, o_r, lambda q: None)
    scales = c_send[...]
    for d in range(1, n_tp):
        peer = lax.rem(tp + d, n_tp)
        pltpu.make_async_remote_copy(
            src_ref=c_send, dst_ref=c_recv.at[peer], send_sem=c_s.at[peer], recv_sem=c_r.at[peer],
            device_id={"tp": peer}, device_id_type=MESH).wait_recv()
        scales = scales + c_recv[peer]
    scale_out[...] = scales
    for part, out in ((0, resid_out), (1, scaled_out)):
        for q in range(n_tp):
            b_rows[q * seqs : (q + 1) * seqs, :] = o_recv[q, part].astype(F32)
        out[...] = b_rows[...].astype(BF16)
    for copy in pending:
        copy.wait_send()


def finish(resid, scaled, scale, resid_out, scaled_out, scale_out):
    resid_out[...] = resid[...]
    scaled_out[...] = scaled[...]
    scale_out[...] = scale[0:1, : scale_out.shape[1]]


def fused(n_dp, n_tp, hidden, w_qkv, w_out, norm_gain, kv_cache, lengths):
    rows, width = hidden.shape
    seqs, kvh, ctx, hd2 = kv_cache.shape
    hd = hd2 // 2
    depth, cols = w_qkv.shape
    odepth, ocols = w_out.shape
    heads = odepth * n_tp // hd
    owide = width // n_tp
    chips = n_dp // 2
    vm = pltpu.VMEM
    dma = pltpu.SemaphoreType.DMA
    all_rows = seqs * heads
    scratch = [
        vm((2, chips, rows, depth), BF16), vm((depth, cols), BF16), vm((odepth, ocols), BF16),
        vm(kv_cache.shape, BF16), vm((rows, width), BF16), vm((rows, width), F32),
        vm((chips, rows, cols), BF16), vm((chips, rows, cols), BF16), vm((chips, rows, cols), F32),
        vm((chips, rows, cols), BF16), vm((chips, rows, cols), BF16), vm((rows, cols), F32),
        vm((n_tp, seqs, cols), BF16), vm((n_tp, seqs, cols), BF16),
        vm((all_rows, hd), F32), vm((all_rows, hd), F32), vm((all_rows, hd), F32), vm((all_rows, hd), F32),
        vm((all_rows, ctx), F32), vm((all_rows, hd), F32),
        vm((n_tp, seqs, odepth), BF16), vm((n_tp, seqs, odepth), BF16), vm((rows, odepth), F32),
        vm((2, chips, rows, odepth), BF16), vm((2, chips, rows, ocols), F32),
        vm((n_tp, 2, chips * seqs, ocols), F32), vm((n_tp, 2, chips * seqs, ocols), BF16),
        vm((n_tp, 2, chips * seqs, ocols), BF16),
        vm((n_dp, seqs, ocols), BF16), vm((n_dp, seqs, ocols), BF16),
        vm((n_tp, 2, seqs, owide), BF16), vm((n_tp, 2, seqs, owide), BF16),
        vm((8, hd), F32), vm((n_tp, 8, hd), F32), vm((seqs, width), F32),
        dma((5,)), dma((n_dp,)), dma((n_dp,)), dma, dma, dma((chips,)), dma((chips,)),
        dma((n_tp,)), dma((n_tp,)), dma((n_tp,)), dma((n_tp,)),
        dma((chips,)), dma((2, chips)), dma((chips,)), dma((n_tp, 2)), dma((n_tp, 2)),
        dma((n_dp,)), dma((n_dp,)), dma((n_tp,)), dma((n_tp,)), dma((n_tp,)), dma((n_tp,)),
    ]
    anywhere = pl.BlockSpec(memory_space=pl.ANY)
    in_vmem = pl.BlockSpec(memory_space=pltpu.VMEM)
    resid, scaled, scale = pl.pallas_call(
        functools.partial(layer, n_dp, n_tp),
        out_shape=(
            jax.ShapeDtypeStruct((rows, owide), BF16),
            jax.ShapeDtypeStruct((rows, owide), BF16),
            jax.ShapeDtypeStruct((8, hd), F32),
        ),
        in_specs=[anywhere, anywhere, anywhere, in_vmem, anywhere, pl.BlockSpec(memory_space=pltpu.SMEM)],
        out_specs=(in_vmem, in_vmem, in_vmem),
        scratch_shapes=scratch,
        compiler_params=pltpu.CompilerParams(
            collective_id=0, has_side_effects=True, vmem_limit_bytes=66_000_000),
    )(hidden, w_qkv, w_out, norm_gain.reshape(1, width), kv_cache, lengths)
    resid, scaled, scale = pl.pallas_call(
        finish,
        out_shape=(
            jax.ShapeDtypeStruct((rows, owide), BF16),
            jax.ShapeDtypeStruct((rows, owide), BF16),
            jax.ShapeDtypeStruct((1, rows), F32),
        ),
        in_specs=[in_vmem, in_vmem, in_vmem],
        out_specs=(in_vmem, in_vmem, in_vmem),
    )(resid, scaled, scale)
    return resid, scaled, scale.reshape(rows)


def solution(mesh):
    placed = (
        P("dp", None),
        P("dp", "tp"),
        P("tp", "dp"),
        P(),
        P(("dp", "tp"), None, None, None),
        P(("dp", "tp")),
    )
    n_dp, n_tp = mesh.shape["dp"], mesh.shape["tp"]

    def body(hidden, w_qkv, w_out, norm_gain, kv_cache, lengths):
        lanes = kv_cache.shape[3] // 2
        fits = (
            n_dp % 2 == 0
            and kv_cache.shape[2] == lanes
            and w_qkv.shape[1] % lanes == 0
            and w_out.shape[0] % lanes == 0
            and w_out.shape[1] % lanes == 0
            and hidden.shape[0] <= lanes
            and hidden.shape[1] // n_tp == w_out.shape[0]
        )
        if fits:
            return fused(n_dp, n_tp, hidden, w_qkv, w_out, norm_gain, kv_cache, lengths)
        return shards(hidden, w_qkv, w_out, norm_gain, kv_cache, lengths)

    return jax.shard_map(
        body,
        mesh=mesh,
        in_specs=placed,
        out_specs=(P("dp", "tp"), P("dp", "tp"), P("dp")),
        check_vma=False,
    )
```

```python
import functools

import jax
import jax.numpy as jnp
from jax import lax
from jax.experimental import pallas as pl
from jax.experimental.pallas import tpu as pltpu
from jax.sharding import PartitionSpec as P


def rope(values, positions):
    half = values.shape[-1] // 2
    freqs = 1000000.0 ** (-2.0 * jnp.arange(half, dtype=jnp.float32) / values.shape[-1])
    angle = positions[..., None] * freqs
    cosine = jnp.cos(angle)
    sine = jnp.sin(angle)
    first = values[..., :half]
    second = values[..., half:]
    return jnp.concatenate(
        [first * cosine - second * sine, second * cosine + first * sine], axis=-1
    )


def shards(hidden, w_qkv, w_out, norm_gain, kv_cache, lengths):
    seq_dev = kv_cache.shape[0]
    kv_heads = kv_cache.shape[1]
    head_size = kv_cache.shape[3] // 2
    tp_count = lax.axis_size("tp")
    w_cols = lax.all_gather(w_qkv, "dp", axis=0, tiled=True)
    qkv_part = jnp.dot(hidden, w_cols, preferred_element_type=jnp.float32)
    mine = lax.all_to_all(
        qkv_part.astype(jnp.bfloat16), "tp", split_axis=0, concat_axis=1, tiled=True
    )
    att_width = w_out.shape[0] * tp_count
    heads = att_width // head_size
    groups = heads // kv_heads
    positions = lengths.astype(jnp.float32)[:, None]
    query = rope(
        mine[:, :att_width].reshape(seq_dev, heads, head_size).astype(jnp.float32), positions
    ).astype(jnp.bfloat16)
    key_new = rope(
        mine[:, att_width : att_width + kv_heads * head_size]
        .reshape(seq_dev, kv_heads, head_size)
        .astype(jnp.float32),
        positions,
    ).astype(jnp.bfloat16)
    value_new = mine[:, att_width + kv_heads * head_size :].reshape(seq_dev, kv_heads, head_size)
    q_grp = query.reshape(seq_dev, kv_heads, groups, head_size)
    keys = kv_cache[..., :head_size]
    vals = kv_cache[..., head_size:]
    scale = 1.0 / head_size**0.5
    scores = jnp.einsum("nkgd,nkpd->nkgp", q_grp, keys, preferred_element_type=jnp.float32) * scale
    own = jnp.einsum("nkgd,nkd->nkg", q_grp, key_new, preferred_element_type=jnp.float32) * scale
    valid = (jnp.arange(kv_cache.shape[2])[None, :] < lengths[:, None])[:, None, None, :]
    scores = jnp.where(valid, scores, jnp.float32(-1e30))
    top = jnp.maximum(jnp.max(scores, axis=-1), own)
    probs = jnp.where(valid, jnp.exp(scores - top[..., None]), jnp.float32(0.0))
    own_prob = jnp.exp(own - top)
    denom = jnp.sum(probs, axis=-1) + own_prob
    weights = (probs / denom[..., None]).astype(jnp.bfloat16)
    own_weight = (own_prob / denom).astype(jnp.bfloat16)
    mixed = jnp.einsum("nkgp,nkpd->nkgd", weights, vals, preferred_element_type=jnp.float32)
    mixed = (
        mixed
        + own_weight.astype(jnp.float32)[..., None] * value_new.astype(jnp.float32)[:, :, None, :]
    )
    attn = mixed.reshape(seq_dev, att_width).astype(jnp.bfloat16)
    heads_part = lax.all_to_all(attn, "tp", split_axis=1, concat_axis=0, tiled=True)
    terms = jnp.dot(
        heads_part,
        lax.all_gather(w_out, "dp", axis=1, tiled=True),
        preferred_element_type=jnp.float32,
    )
    width = terms.shape[1]
    share = width // tp_count
    offset = lax.axis_index("tp") * share
    summed = lax.psum_scatter(
        terms.astype(jnp.bfloat16), "tp", scatter_dimension=1, tiled=True
    ).astype(jnp.float32)
    hidden_mine = lax.dynamic_slice_in_dim(hidden, offset, share, 1).astype(jnp.float32)
    gain_mine = lax.dynamic_slice_in_dim(norm_gain, offset, share, 0)
    resid_mine = hidden_mine + summed
    weighted = resid_mine * gain_mine[None, :]
    squares = lax.psum(jnp.sum(resid_mine * resid_mine, axis=-1), "tp")
    peak = lax.pmax(jnp.max(jnp.abs(weighted), axis=-1), "tp")
    inverse = lax.rsqrt(squares / width + 1e-06)
    normed_mine = weighted * inverse[:, None]
    row_scale = (peak * inverse + 1e-06) / 448.0
    residual_out = resid_mine.astype(jnp.bfloat16)
    scaled = (normed_mine / row_scale[:, None]).astype(jnp.bfloat16)
    return (residual_out, scaled, row_scale)


F32 = jnp.float32
BF16 = jnp.bfloat16
MESH = pl.DeviceIdType.MESH


def send(src, dst, send_sem, recv_sem, where):
    copy = pltpu.make_async_remote_copy(
        src_ref=src, dst_ref=dst, send_sem=send_sem, recv_sem=recv_sem,
        device_id=where, device_id_type=MESH,
    )
    copy.start()
    return copy


def layer(
    n_dp, n_tp,
    hidden, w_qkv, w_out, gain, cache, lens,
    resid_out, scaled_out, scale_out,
    h_all, w1, w2, kv, hid, hid32, p_send, p_recv, r_acc, r_send, r_recv, mine32,
    t1_send, t1_recv, q_rows, k_rows, v_rows, l_rows, s_rows, a_rows,
    t2_send, t2_recv, b_rows, ag, mm, mq, t3_send, t3_recv, f_send, f_recv,
    o_send, o_recv, c_send, c_recv, fin,
    loc_sem, h_s, h_r, p_s, p_r, r_s, r_r, t1_s, t1_r, t2_s, t2_r,
    g_s, g_r, x_s, t3_s, t3_r, f_s, f_r, o_s, o_r, c_s, c_r,
):
    dp = lax.axis_index("dp")
    tp = lax.axis_index("tp")
    core = lax.rem(dp, 2)
    chip = dp // 2
    other = 1 - core
    partner = chip * 2 + other
    n_chip = n_dp // 2
    rows = hidden.shape[0]
    seqs = rows // n_tp
    depth = w_qkv.shape[0]
    ocols = w_out.shape[1]
    owide = resid_out.shape[1]
    kvh = cache.shape[1]
    ctx = cache.shape[2]
    hd = cache.shape[3] // 2
    heads = (w_out.shape[0] * n_tp) // hd
    groups = heads // kvh
    per = w_qkv.shape[1] // hd
    per_out = w_out.shape[0] // hd
    width = hidden.shape[1]

    own_h = pltpu.make_async_copy(
        hidden.at[:, pl.ds(pl.multiple_of(dp * depth, depth), depth)], h_all.at[core, chip], loc_sem.at[0])
    own_h.start()
    load_w1 = pltpu.make_async_copy(w_qkv, w1, loc_sem.at[1])
    load_w1.start()

    barrier = pltpu.get_barrier_semaphore()
    for d in range(1, n_dp):
        pl.semaphore_signal(barrier, inc=1, device_id={"dp": lax.rem(dp + d, n_dp)}, device_id_type=MESH)
    for d in range(1, n_tp):
        pl.semaphore_signal(barrier, inc=1, device_id={"tp": lax.rem(tp + d, n_tp)}, device_id_type=MESH)
    pl.semaphore_wait(barrier, n_dp + n_tp - 2)

    pending = []
    for d in [*range(1, n_dp, 2), *range(2, n_dp, 2)]:
        peer = lax.rem(dp + d, n_dp)
        pending.append(send(
            hidden.at[:, pl.ds(pl.multiple_of(peer * depth, depth), depth)],
            h_all.at[core, chip], h_s.at[peer], h_r.at[dp], {"dp": peer}))
    load_kv = pltpu.make_async_copy(cache, kv, loc_sem.at[2])
    load_kv.start()
    load_w2 = pltpu.make_async_copy(w_out, w2, loc_sem.at[3])
    load_w2.start()
    load_hid = pltpu.make_async_copy(hidden, hid, loc_sem.at[4])
    load_hid.start()

    row_i = lax.broadcasted_iota(jnp.int32, (seqs, hd), 0)
    lane_i = lax.broadcasted_iota(jnp.int32, (seqs, hd), 1)
    live = jnp.zeros((seqs, hd), jnp.int32)
    for n in range(seqs):
        live = jnp.where(row_i == n, lens[n], live)
    half = hd // 2
    low = lane_i < half
    index = jnp.where(low, lane_i, lane_i - half).astype(F32)
    freqs = jnp.exp(index * F32(-2.0 * 13.815510557964274 / hd))
    angle = live.astype(F32) * freqs
    cosine = jnp.cos(angle)
    sine = jnp.where(low, -jnp.sin(angle), jnp.sin(angle))
    for h in range(heads):
        l_rows[pl.ds(h, seqs, stride=heads), :] = live.astype(F32)
    load_hid.wait()
    hid32[...] = hid[...].astype(F32)
    for r in range(n_dp):
        block = slice(r * ocols, (r + 1) * ocols)
        mine = hid32[0:seqs, block]
        for q in range(1, n_tp):
            mine = jnp.where(tp == q, hid32[q * seqs : (q + 1) * seqs, block], mine)
        fin[:, block] = mine

    def recv_h(peer):
        pltpu.make_async_remote_copy(
            src_ref=h_all.at[core, chip], dst_ref=h_all.at[lax.rem(peer, 2), peer // 2],
            send_sem=h_s.at[peer], recv_sem=h_r.at[peer],
            device_id={"dp": peer}, device_id_type=MESH).wait_recv()

    own_h.wait()
    load_w1.wait()
    for d in range(n_chip):
        recv_h(2 * d + other)
    part = jnp.dot(h_all[other].reshape(n_chip * rows, depth), w1[...], preferred_element_type=F32)
    p_send[...] = part.astype(BF16).reshape(p_send.shape)
    swap = send(p_send, p_recv, p_s, p_r, {"dp": partner})
    pending.append(swap)
    for d in range(1, n_chip):
        recv_h(2 * lax.rem(chip + d, n_chip) + core)
    part = jnp.dot(h_all[core].reshape(n_chip * rows, depth), w1[...], preferred_element_type=F32)
    r_acc[...] = part.reshape(r_acc.shape)
    swap.wait_recv()
    for d in range(1, n_chip):
        to = lax.rem(chip + d, n_chip)
        r_send[to] = (r_acc[to] + p_recv[to].astype(F32)).astype(BF16)
        pending.append(send(r_send.at[to], r_recv.at[chip], r_s.at[to], r_r.at[chip], {"dp": to * 2 + core}))
    total = r_acc[chip] + p_recv[chip].astype(F32)
    for d in range(1, n_chip):
        who = lax.rem(chip + d, n_chip)
        pltpu.make_async_remote_copy(
            src_ref=r_send.at[who], dst_ref=r_recv.at[who], send_sem=r_s.at[who], recv_sem=r_r.at[who],
            device_id={"dp": who * 2 + core}, device_id_type=MESH).wait_recv()
        total = total + r_recv[who].astype(F32)
    mine32[...] = total

    def exchange(src, dst, s_sem, r_sem, fill):
        for q in range(n_tp):
            fill(q)
        keep = pltpu.make_async_copy(src.at[tp], dst.at[tp], r_sem.at[tp])
        keep.start()
        sent = []
        for d in range(1, n_tp):
            peer = lax.rem(tp + d, n_tp)
            sent.append(send(src.at[peer], dst.at[tp], s_sem.at[peer], r_sem.at[tp], {"tp": peer}))
        keep.wait()
        for d in range(1, n_tp):
            peer = lax.rem(tp + d, n_tp)
            pltpu.make_async_remote_copy(
                src_ref=src.at[peer], dst_ref=dst.at[peer], send_sem=s_sem.at[peer], recv_sem=r_sem.at[peer],
                device_id={"tp": peer}, device_id_type=MESH).wait_recv()
        return sent

    def fill1(q):
        t1_send[q] = mine32[q * seqs : (q + 1) * seqs, :].astype(BF16)

    pending += exchange(t1_send, t1_recv, t1_s, t1_r, fill1)

    def head(h):
        return t1_recv[h // per, :, (h % per) * hd : (h % per + 1) * hd].astype(F32)

    def turn(x):
        return (x * cosine + pltpu.roll(x, half, 1) * sine).astype(BF16).astype(F32)

    for h in range(heads):
        q_rows[pl.ds(h, seqs, stride=heads), :] = turn(head(h))
    for k in range(kvh):
        key_new = turn(head(heads + k))
        value_new = head(heads + kvh + k)
        for g in range(groups):
            k_rows[pl.ds(k * groups + g, seqs, stride=heads), :] = key_new
            v_rows[pl.ds(k * groups + g, seqs, stride=heads), :] = value_new
    load_kv.wait()
    for n in range(seqs):
        for k in range(kvh):
            at = (n * kvh + k) * groups
            s_rows[at : at + groups, :] = lax.dot_general(
                q_rows[at : at + groups, :].astype(BF16), kv[n, k, :, :hd],
                (((1,), (1,)), ((), ())), preferred_element_type=F32)
    factor = F32(1.0 / hd**0.5)
    pos = lax.broadcasted_iota(jnp.int32, (seqs * heads, ctx), 1).astype(F32)
    valid = pos < l_rows[...]
    scores = jnp.where(valid, s_rows[...] * factor, F32(-1e30))
    own = jnp.sum(q_rows[...] * k_rows[...], axis=1, keepdims=True) * factor
    top = jnp.maximum(jnp.max(scores, axis=1, keepdims=True), own)
    probs = jnp.where(valid, jnp.exp(scores - top), F32(0.0))
    own_prob = jnp.exp(own - top)
    denom = jnp.sum(probs, axis=1, keepdims=True) + own_prob
    s_rows[...] = probs / denom
    own_weight = (own_prob / denom).astype(BF16).astype(F32)
    v_rows[...] = own_weight * v_rows[...]
    for n in range(seqs):
        for k in range(kvh):
            at = (n * kvh + k) * groups
            a_rows[at : at + groups, :] = jnp.dot(
                s_rows[at : at + groups, :].astype(BF16), kv[n, k, :, hd:],
                preferred_element_type=F32) + v_rows[at : at + groups, :]

    def fill2(q):
        for e in range(per_out):
            t2_send[q, :, e * hd : (e + 1) * hd] = a_rows[
                pl.ds(q * per_out + e, seqs, stride=heads), :].astype(BF16)

    pending += exchange(t2_send, t2_recv, t2_s, t2_r, fill2)
    for q in range(n_tp):
        b_rows[q * seqs : (q + 1) * seqs, :] = t2_recv[q].astype(F32)
    ag[core, chip] = b_rows[...].astype(BF16)
    for d in range(1, n_chip):
        to = lax.rem(chip + d, n_chip)
        pending.append(send(ag.at[core, chip], ag.at[core, chip], g_s.at[to], g_r.at[core, chip],
                            {"dp": to * 2 + core}))
    pending.append(send(ag.at[core, chip], ag.at[core, chip], x_s.at[chip], g_r.at[core, chip], {"dp": partner}))

    def recv_g(c, who):
        pltpu.make_async_remote_copy(
            src_ref=ag.at[core, chip], dst_ref=ag.at[c, who], send_sem=x_s.at[chip], recv_sem=g_r.at[c, who],
            device_id={"dp": partner}, device_id_type=MESH).wait_recv()

    for d in range(1, n_chip):
        who = lax.rem(chip + d, n_chip)
        recv_g(core, who)
        pending.append(send(ag.at[core, who], ag.at[core, who], x_s.at[who], g_r.at[core, who], {"dp": partner}))
    load_w2.wait()
    def project(side):
        mm[side] = jnp.dot(ag[side].reshape(n_chip * rows, w_out.shape[0]), w2[...],
                           preferred_element_type=F32).reshape(n_chip, rows, ocols)
        for q in range(n_tp):
            for c in range(n_chip):
                mq[q, side, c * seqs : (c + 1) * seqs, :] = mm[side, c, q * seqs : (q + 1) * seqs, :]
            t3_send[q, side] = mq[q, side].astype(BF16)
        for d in range(1, n_tp):
            peer = lax.rem(tp + d, n_tp)
            pending.append(send(
                t3_send.at[peer, side], t3_recv.at[tp, side], t3_s.at[peer, side], t3_r.at[tp, side],
                {"tp": peer}))

    def scatter(side):
        total = t3_send[tp, side].astype(F32)
        for d in range(1, n_tp):
            peer = lax.rem(tp + d, n_tp)
            pltpu.make_async_remote_copy(
                src_ref=t3_send.at[peer, side], dst_ref=t3_recv.at[peer, side],
                send_sem=t3_s.at[peer, side], recv_sem=t3_r.at[peer, side],
                device_id={"tp": peer}, device_id_type=MESH).wait_recv()
            total = total + t3_recv[peer, side].astype(F32)
        mq[0, side] = total
        for c in range(n_chip):
            f_send[2 * c + side] = mq[0, side, c * seqs : (c + 1) * seqs, :].astype(BF16)
        for d in range(n_chip):
            to = 2 * lax.rem(chip + d, n_chip) + side
            if d or side is not core:
                pending.append(send(f_send.at[to], f_recv.at[dp], f_s.at[to], f_r.at[dp], {"dp": to}))
            else:
                pltpu.make_async_copy(f_send.at[dp], f_recv.at[dp], loc_sem.at[0]).start()

    project(core)
    for d in range(n_chip):
        recv_g(other, d)
    project(other)
    scatter(core)
    scatter(other)
    pltpu.make_async_copy(f_send.at[dp], f_recv.at[dp], loc_sem.at[0]).wait()
    for d in range(1, n_dp):
        peer = lax.rem(dp + d, n_dp)
        pltpu.make_async_remote_copy(
            src_ref=f_send.at[peer], dst_ref=f_recv.at[peer], send_sem=f_s.at[peer], recv_sem=f_r.at[peer],
            device_id={"dp": peer}, device_id_type=MESH).wait_recv()
    for r in range(n_dp):
        block = slice(r * ocols, (r + 1) * ocols)
        fin[:, block] = fin[:, block] + f_recv[r].astype(F32)
    resid = fin[...]
    inverse = lax.rsqrt(jnp.sum(resid * resid, axis=1, keepdims=True) / width + F32(1e-06))
    weighted = resid * gain[...]
    peak = jnp.max(jnp.abs(weighted), axis=1, keepdims=True)
    scale = (peak * inverse + F32(1e-06)) / F32(448.0)
    scaled = (weighted * (inverse / scale)).astype(BF16)
    for q in range(n_tp):
        o_send[q, 0] = resid[:, q * owide : (q + 1) * owide].astype(BF16)
        o_send[q, 1] = scaled[:, q * owide : (q + 1) * owide]
    spread = jnp.where(lane_i == row_i + tp * seqs, jnp.broadcast_to(scale, lane_i.shape), F32(0.0))
    c_send[...] = jnp.broadcast_to(jnp.sum(spread, axis=0, keepdims=True), c_send.shape)
    for d in range(1, n_tp):
        peer = lax.rem(tp + d, n_tp)
        pending.append(send(c_send, c_recv.at[tp], c_s.at[peer], c_r.at[tp], {"tp": peer}))
    pending += exchange(o_send, o_recv, o_s, o_r, lambda q: None)
    scales = c_send[...]
    for d in range(1, n_tp):
        peer = lax.rem(tp + d, n_tp)
        pltpu.make_async_remote_copy(
            src_ref=c_send, dst_ref=c_recv.at[peer], send_sem=c_s.at[peer], recv_sem=c_r.at[peer],
            device_id={"tp": peer}, device_id_type=MESH).wait_recv()
        scales = scales + c_recv[peer]
    scale_out[...] = scales
    for part, out in ((0, resid_out), (1, scaled_out)):
        for q in range(n_tp):
            b_rows[q * seqs : (q + 1) * seqs, :] = o_recv[q, part].astype(F32)
        out[...] = b_rows[...].astype(BF16)
    for copy in pending:
        copy.wait_send()


def finish(resid, scaled, scale, resid_out, scaled_out, scale_out):
    resid_out[...] = resid[...]
    scaled_out[...] = scaled[...]
    scale_out[...] = scale[0:1, : scale_out.shape[1]]


def fused(n_dp, n_tp, hidden, w_qkv, w_out, norm_gain, kv_cache, lengths):
    rows, width = hidden.shape
    seqs, kvh, ctx, hd2 = kv_cache.shape
    hd = hd2 // 2
    depth, cols = w_qkv.shape
    odepth, ocols = w_out.shape
    heads = odepth * n_tp // hd
    owide = width // n_tp
    chips = n_dp // 2
    vm = pltpu.VMEM
    dma = pltpu.SemaphoreType.DMA
    all_rows = seqs * heads
    scratch = [
        vm((2, chips, rows, depth), BF16), vm((depth, cols), BF16), vm((odepth, ocols), BF16),
        vm(kv_cache.shape, BF16), vm((rows, width), BF16), vm((rows, width), F32),
        vm((chips, rows, cols), BF16), vm((chips, rows, cols), BF16), vm((chips, rows, cols), F32),
        vm((chips, rows, cols), BF16), vm((chips, rows, cols), BF16), vm((rows, cols), F32),
        vm((n_tp, seqs, cols), BF16), vm((n_tp, seqs, cols), BF16),
        vm((all_rows, hd), F32), vm((all_rows, hd), F32), vm((all_rows, hd), F32), vm((all_rows, hd), F32),
        vm((all_rows, ctx), F32), vm((all_rows, hd), F32),
        vm((n_tp, seqs, odepth), BF16), vm((n_tp, seqs, odepth), BF16), vm((rows, odepth), F32),
        vm((2, chips, rows, odepth), BF16), vm((2, chips, rows, ocols), F32),
        vm((n_tp, 2, chips * seqs, ocols), F32), vm((n_tp, 2, chips * seqs, ocols), BF16),
        vm((n_tp, 2, chips * seqs, ocols), BF16),
        vm((n_dp, seqs, ocols), BF16), vm((n_dp, seqs, ocols), BF16),
        vm((n_tp, 2, seqs, owide), BF16), vm((n_tp, 2, seqs, owide), BF16),
        vm((8, hd), F32), vm((n_tp, 8, hd), F32), vm((seqs, width), F32),
        dma((5,)), dma((n_dp,)), dma((n_dp,)), dma, dma, dma((chips,)), dma((chips,)),
        dma((n_tp,)), dma((n_tp,)), dma((n_tp,)), dma((n_tp,)),
        dma((chips,)), dma((2, chips)), dma((chips,)), dma((n_tp, 2)), dma((n_tp, 2)),
        dma((n_dp,)), dma((n_dp,)), dma((n_tp,)), dma((n_tp,)), dma((n_tp,)), dma((n_tp,)),
    ]
    anywhere = pl.BlockSpec(memory_space=pl.ANY)
    in_vmem = pl.BlockSpec(memory_space=pltpu.VMEM)
    resid, scaled, scale = pl.pallas_call(
        functools.partial(layer, n_dp, n_tp),
        out_shape=(
            jax.ShapeDtypeStruct((rows, owide), BF16),
            jax.ShapeDtypeStruct((rows, owide), BF16),
            jax.ShapeDtypeStruct((8, hd), F32),
        ),
        in_specs=[anywhere, anywhere, anywhere, in_vmem, anywhere, pl.BlockSpec(memory_space=pltpu.SMEM)],
        out_specs=(in_vmem, in_vmem, in_vmem),
        scratch_shapes=scratch,
        compiler_params=pltpu.CompilerParams(
            collective_id=0, has_side_effects=True, vmem_limit_bytes=66_000_000),
    )(hidden, w_qkv, w_out, norm_gain.reshape(1, width), kv_cache, lengths)
    resid, scaled, scale = pl.pallas_call(
        finish,
        out_shape=(
            jax.ShapeDtypeStruct((rows, owide), BF16),
            jax.ShapeDtypeStruct((rows, owide), BF16),
            jax.ShapeDtypeStruct((1, rows), F32),
        ),
        in_specs=[in_vmem, in_vmem, in_vmem],
        out_specs=(in_vmem, in_vmem, in_vmem),
    )(resid, scaled, scale)
    return resid, scaled, scale.reshape(rows)


def solution(mesh):
    placed = (
        P("dp", None),
        P("dp", "tp"),
        P("tp", "dp"),
        P(),
        P(("dp", "tp"), None, None, None),
        P(("dp", "tp")),
    )
    n_dp, n_tp = mesh.shape["dp"], mesh.shape["tp"]

    def body(hidden, w_qkv, w_out, norm_gain, kv_cache, lengths):
        lanes = kv_cache.shape[3] // 2
        fits = (
            n_dp % 2 == 0
            and kv_cache.shape[2] == lanes
            and w_qkv.shape[1] % lanes == 0
            and w_out.shape[0] % lanes == 0
            and w_out.shape[1] % lanes == 0
            and hidden.shape[0] <= lanes
            and hidden.shape[1] // n_tp == w_out.shape[0]
        )
        if fits:
            return fused(n_dp, n_tp, hidden, w_qkv, w_out, norm_gain, kv_cache, lengths)
        return shards(hidden, w_qkv, w_out, norm_gain, kv_cache, lengths)

    return jax.shard_map(
        body,
        mesh=mesh,
        in_specs=placed,
        out_specs=(P("dp", "tp"), P("dp", "tp"), P("dp")),
        check_vma=False,
    )
```

```python
import functools

import jax
import jax.numpy as jnp
from jax import lax
from jax.experimental import pallas as pl
from jax.experimental.pallas import tpu as pltpu
from jax.sharding import PartitionSpec as P


def rope(values, positions):
    half = values.shape[-1] // 2
    freqs = 1000000.0 ** (-2.0 * jnp.arange(half, dtype=jnp.float32) / values.shape[-1])
    angle = positions[..., None] * freqs
    cosine = jnp.cos(angle)
    sine = jnp.sin(angle)
    first = values[..., :half]
    second = values[..., half:]
    return jnp.concatenate(
        [first * cosine - second * sine, second * cosine + first * sine], axis=-1
    )


def shards(hidden, w_qkv, w_out, norm_gain, kv_cache, lengths):
    seq_dev = kv_cache.shape[0]
    kv_heads = kv_cache.shape[1]
    head_size = kv_cache.shape[3] // 2
    tp_count = lax.axis_size("tp")
    w_cols = lax.all_gather(w_qkv, "dp", axis=0, tiled=True)
    qkv_part = jnp.dot(hidden, w_cols, preferred_element_type=jnp.float32)
    mine = lax.all_to_all(
        qkv_part.astype(jnp.bfloat16), "tp", split_axis=0, concat_axis=1, tiled=True
    )
    att_width = w_out.shape[0] * tp_count
    heads = att_width // head_size
    groups = heads // kv_heads
    positions = lengths.astype(jnp.float32)[:, None]
    query = rope(
        mine[:, :att_width].reshape(seq_dev, heads, head_size).astype(jnp.float32), positions
    ).astype(jnp.bfloat16)
    key_new = rope(
        mine[:, att_width : att_width + kv_heads * head_size]
        .reshape(seq_dev, kv_heads, head_size)
        .astype(jnp.float32),
        positions,
    ).astype(jnp.bfloat16)
    value_new = mine[:, att_width + kv_heads * head_size :].reshape(seq_dev, kv_heads, head_size)
    q_grp = query.reshape(seq_dev, kv_heads, groups, head_size)
    keys = kv_cache[..., :head_size]
    vals = kv_cache[..., head_size:]
    scale = 1.0 / head_size**0.5
    scores = jnp.einsum("nkgd,nkpd->nkgp", q_grp, keys, preferred_element_type=jnp.float32) * scale
    own = jnp.einsum("nkgd,nkd->nkg", q_grp, key_new, preferred_element_type=jnp.float32) * scale
    valid = (jnp.arange(kv_cache.shape[2])[None, :] < lengths[:, None])[:, None, None, :]
    scores = jnp.where(valid, scores, jnp.float32(-1e30))
    top = jnp.maximum(jnp.max(scores, axis=-1), own)
    probs = jnp.where(valid, jnp.exp(scores - top[..., None]), jnp.float32(0.0))
    own_prob = jnp.exp(own - top)
    denom = jnp.sum(probs, axis=-1) + own_prob
    weights = (probs / denom[..., None]).astype(jnp.bfloat16)
    own_weight = (own_prob / denom).astype(jnp.bfloat16)
    mixed = jnp.einsum("nkgp,nkpd->nkgd", weights, vals, preferred_element_type=jnp.float32)
    mixed = (
        mixed
        + own_weight.astype(jnp.float32)[..., None] * value_new.astype(jnp.float32)[:, :, None, :]
    )
    attn = mixed.reshape(seq_dev, att_width).astype(jnp.bfloat16)
    heads_part = lax.all_to_all(attn, "tp", split_axis=1, concat_axis=0, tiled=True)
    terms = jnp.dot(
        heads_part,
        lax.all_gather(w_out, "dp", axis=1, tiled=True),
        preferred_element_type=jnp.float32,
    )
    width = terms.shape[1]
    share = width // tp_count
    offset = lax.axis_index("tp") * share
    summed = lax.psum_scatter(
        terms.astype(jnp.bfloat16), "tp", scatter_dimension=1, tiled=True
    ).astype(jnp.float32)
    hidden_mine = lax.dynamic_slice_in_dim(hidden, offset, share, 1).astype(jnp.float32)
    gain_mine = lax.dynamic_slice_in_dim(norm_gain, offset, share, 0)
    resid_mine = hidden_mine + summed
    weighted = resid_mine * gain_mine[None, :]
    squares = lax.psum(jnp.sum(resid_mine * resid_mine, axis=-1), "tp")
    peak = lax.pmax(jnp.max(jnp.abs(weighted), axis=-1), "tp")
    inverse = lax.rsqrt(squares / width + 1e-06)
    normed_mine = weighted * inverse[:, None]
    row_scale = (peak * inverse + 1e-06) / 448.0
    residual_out = resid_mine.astype(jnp.bfloat16)
    scaled = (normed_mine / row_scale[:, None]).astype(jnp.bfloat16)
    return (residual_out, scaled, row_scale)


F32 = jnp.float32
BF16 = jnp.bfloat16
MESH = pl.DeviceIdType.MESH


def send(src, dst, send_sem, recv_sem, where):
    copy = pltpu.make_async_remote_copy(
        src_ref=src, dst_ref=dst, send_sem=send_sem, recv_sem=recv_sem,
        device_id=where, device_id_type=MESH,
    )
    copy.start()
    return copy


def layer(
    n_dp, n_tp,
    hidden, w_qkv, w_out, gain, cache, lens,
    resid_out, scaled_out, scale_out,
    h_all, w1, w2, kv, hid, hid32, p_send, p_recv, r_acc, r_send, r_recv, mine32,
    t1_send, t1_recv, q_rows, k_rows, v_rows, l_rows, s_rows, a_rows,
    t2_send, t2_recv, b_rows, ag, mm, mq, t3_send, t3_recv, f_send, f_recv,
    o_send, o_recv, c_send, c_recv, fin,
    loc_sem, h_s, h_r, p_s, p_r, r_s, r_r, t1_s, t1_r, t2_s, t2_r,
    g_s, g_r, x_s, t3_s, t3_r, f_s, f_r, o_s, o_r, c_s, c_r,
):
    dp = lax.axis_index("dp")
    tp = lax.axis_index("tp")
    core = lax.rem(dp, 2)
    chip = dp // 2
    other = 1 - core
    partner = chip * 2 + other
    n_chip = n_dp // 2
    rows = hidden.shape[0]
    seqs = rows // n_tp
    depth = w_qkv.shape[0]
    ocols = w_out.shape[1]
    owide = resid_out.shape[1]
    kvh = cache.shape[1]
    ctx = cache.shape[2]
    hd = cache.shape[3] // 2
    heads = (w_out.shape[0] * n_tp) // hd
    groups = heads // kvh
    per = w_qkv.shape[1] // hd
    per_out = w_out.shape[0] // hd
    width = hidden.shape[1]

    load_hid = pltpu.make_async_copy(hidden, hid, loc_sem.at[4])
    load_hid.start()
    own_h = pltpu.make_async_copy(
        hidden.at[:, pl.ds(pl.multiple_of(dp * depth, depth), depth)], h_all.at[core, chip], loc_sem.at[0])
    own_h.start()
    load_w1 = pltpu.make_async_copy(w_qkv, w1, loc_sem.at[1])
    load_w1.start()

    barrier = pltpu.get_barrier_semaphore()
    for d in range(1, n_dp):
        pl.semaphore_signal(barrier, inc=1, device_id={"dp": lax.rem(dp + d, n_dp)}, device_id_type=MESH)
    for d in range(1, n_tp):
        pl.semaphore_signal(barrier, inc=1, device_id={"tp": lax.rem(tp + d, n_tp)}, device_id_type=MESH)
    pl.semaphore_wait(barrier, n_dp + n_tp - 2)

    load_hid.wait()
    pending = []
    for d in [*range(1, n_dp, 2), *range(2, n_dp, 2)]:
        peer = lax.rem(dp + d, n_dp)
        pending.append(send(
            hid.at[:, pl.ds(pl.multiple_of(peer * depth, depth), depth)],
            h_all.at[core, chip], h_s.at[peer], h_r.at[dp], {"dp": peer}))
    load_kv = pltpu.make_async_copy(cache, kv, loc_sem.at[2])
    load_kv.start()
    load_w2 = pltpu.make_async_copy(w_out, w2, loc_sem.at[3])
    load_w2.start()

    row_i = lax.broadcasted_iota(jnp.int32, (seqs, hd), 0)
    lane_i = lax.broadcasted_iota(jnp.int32, (seqs, hd), 1)
    live = jnp.zeros((seqs, hd), jnp.int32)
    for n in range(seqs):
        live = jnp.where(row_i == n, lens[n], live)
    half = hd // 2
    low = lane_i < half
    index = jnp.where(low, lane_i, lane_i - half).astype(F32)
    freqs = jnp.exp(index * F32(-2.0 * 13.815510557964274 / hd))
    angle = live.astype(F32) * freqs
    cosine = jnp.cos(angle)
    sine = jnp.where(low, -jnp.sin(angle), jnp.sin(angle))
    for h in range(heads):
        l_rows[pl.ds(h, seqs, stride=heads), :] = live.astype(F32)
    hid32[...] = hid[...].astype(F32)
    for r in range(n_dp):
        block = slice(r * ocols, (r + 1) * ocols)
        mine = hid32[0:seqs, block]
        for q in range(1, n_tp):
            mine = jnp.where(tp == q, hid32[q * seqs : (q + 1) * seqs, block], mine)
        fin[:, block] = mine

    def recv_h(peer):
        pltpu.make_async_remote_copy(
            src_ref=h_all.at[core, chip], dst_ref=h_all.at[lax.rem(peer, 2), peer // 2],
            send_sem=h_s.at[peer], recv_sem=h_r.at[peer],
            device_id={"dp": peer}, device_id_type=MESH).wait_recv()

    own_h.wait()
    load_w1.wait()
    for d in range(n_chip):
        recv_h(2 * d + other)
    part = jnp.dot(h_all[other].reshape(n_chip * rows, depth), w1[...], preferred_element_type=F32)
    p_send[...] = part.astype(BF16).reshape(p_send.shape)
    swap = send(p_send, p_recv, p_s, p_r, {"dp": partner})
    pending.append(swap)
    for d in range(1, n_chip):
        recv_h(2 * lax.rem(chip + d, n_chip) + core)
    part = jnp.dot(h_all[core].reshape(n_chip * rows, depth), w1[...], preferred_element_type=F32)
    r_acc[...] = part.reshape(r_acc.shape)
    swap.wait_recv()
    for d in range(1, n_chip):
        to = lax.rem(chip + d, n_chip)
        r_send[to] = (r_acc[to] + p_recv[to].astype(F32)).astype(BF16)
        pending.append(send(r_send.at[to], r_recv.at[chip], r_s.at[to], r_r.at[chip], {"dp": to * 2 + core}))
    total = r_acc[chip] + p_recv[chip].astype(F32)
    for d in range(1, n_chip):
        who = lax.rem(chip + d, n_chip)
        pltpu.make_async_remote_copy(
            src_ref=r_send.at[who], dst_ref=r_recv.at[who], send_sem=r_s.at[who], recv_sem=r_r.at[who],
            device_id={"dp": who * 2 + core}, device_id_type=MESH).wait_recv()
        total = total + r_recv[who].astype(F32)
    mine32[...] = total

    def exchange(src, dst, s_sem, r_sem, fill):
        for q in range(n_tp):
            fill(q)
        keep = pltpu.make_async_copy(src.at[tp], dst.at[tp], r_sem.at[tp])
        keep.start()
        sent = []
        for d in range(1, n_tp):
            peer = lax.rem(tp + d, n_tp)
            sent.append(send(src.at[peer], dst.at[tp], s_sem.at[peer], r_sem.at[tp], {"tp": peer}))
        keep.wait()
        for d in range(1, n_tp):
            peer = lax.rem(tp + d, n_tp)
            pltpu.make_async_remote_copy(
                src_ref=src.at[peer], dst_ref=dst.at[peer], send_sem=s_sem.at[peer], recv_sem=r_sem.at[peer],
                device_id={"tp": peer}, device_id_type=MESH).wait_recv()
        return sent

    def fill1(q):
        t1_send[q] = mine32[q * seqs : (q + 1) * seqs, :].astype(BF16)

    pending += exchange(t1_send, t1_recv, t1_s, t1_r, fill1)

    def head(h):
        return t1_recv[h // per, :, (h % per) * hd : (h % per + 1) * hd].astype(F32)

    def turn(x):
        return (x * cosine + pltpu.roll(x, half, 1) * sine).astype(BF16).astype(F32)

    for h in range(heads):
        q_rows[pl.ds(h, seqs, stride=heads), :] = turn(head(h))
    for k in range(kvh):
        key_new = turn(head(heads + k))
        value_new = head(heads + kvh + k)
        for g in range(groups):
            k_rows[pl.ds(k * groups + g, seqs, stride=heads), :] = key_new
            v_rows[pl.ds(k * groups + g, seqs, stride=heads), :] = value_new
    load_kv.wait()
    for n in range(seqs):
        for k in range(kvh):
            at = (n * kvh + k) * groups
            s_rows[at : at + groups, :] = lax.dot_general(
                q_rows[at : at + groups, :].astype(BF16), kv[n, k, :, :hd],
                (((1,), (1,)), ((), ())), preferred_element_type=F32)
    factor = F32(1.0 / hd**0.5)
    pos = lax.broadcasted_iota(jnp.int32, (seqs * heads, ctx), 1).astype(F32)
    valid = pos < l_rows[...]
    scores = jnp.where(valid, s_rows[...] * factor, F32(-1e30))
    own = jnp.sum(q_rows[...] * k_rows[...], axis=1, keepdims=True) * factor
    top = jnp.maximum(jnp.max(scores, axis=1, keepdims=True), own)
    probs = jnp.where(valid, jnp.exp(scores - top), F32(0.0))
    own_prob = jnp.exp(own - top)
    denom = jnp.sum(probs, axis=1, keepdims=True) + own_prob
    s_rows[...] = probs / denom
    own_weight = (own_prob / denom).astype(BF16).astype(F32)
    v_rows[...] = own_weight * v_rows[...]
    for n in range(seqs):
        for k in range(kvh):
            at = (n * kvh + k) * groups
            a_rows[at : at + groups, :] = jnp.dot(
                s_rows[at : at + groups, :].astype(BF16), kv[n, k, :, hd:],
                preferred_element_type=F32) + v_rows[at : at + groups, :]

    def fill2(q):
        for e in range(per_out):
            t2_send[q, :, e * hd : (e + 1) * hd] = a_rows[
                pl.ds(q * per_out + e, seqs, stride=heads), :].astype(BF16)

    pending += exchange(t2_send, t2_recv, t2_s, t2_r, fill2)
    for q in range(n_tp):
        b_rows[q * seqs : (q + 1) * seqs, :] = t2_recv[q].astype(F32)
    ag[core, chip] = b_rows[...].astype(BF16)
    for d in range(1, n_chip):
        to = lax.rem(chip + d, n_chip)
        pending.append(send(ag.at[core, chip], ag.at[core, chip], g_s.at[to], g_r.at[core, chip],
                            {"dp": to * 2 + core}))
    pending.append(send(ag.at[core, chip], ag.at[core, chip], x_s.at[chip], g_r.at[core, chip], {"dp": partner}))

    def recv_g(c, who):
        pltpu.make_async_remote_copy(
            src_ref=ag.at[core, chip], dst_ref=ag.at[c, who], send_sem=x_s.at[chip], recv_sem=g_r.at[c, who],
            device_id={"dp": partner}, device_id_type=MESH).wait_recv()

    for d in range(1, n_chip):
        who = lax.rem(chip + d, n_chip)
        recv_g(core, who)
        pending.append(send(ag.at[core, who], ag.at[core, who], x_s.at[who], g_r.at[core, who], {"dp": partner}))
    load_w2.wait()
    def project(side):
        mm[side] = jnp.dot(ag[side].reshape(n_chip * rows, w_out.shape[0]), w2[...],
                           preferred_element_type=F32).reshape(n_chip, rows, ocols)
        for q in range(n_tp):
            for c in range(n_chip):
                mq[q, side, c * seqs : (c + 1) * seqs, :] = mm[side, c, q * seqs : (q + 1) * seqs, :]
            t3_send[q, side] = mq[q, side].astype(BF16)
        for d in range(1, n_tp):
            peer = lax.rem(tp + d, n_tp)
            pending.append(send(
                t3_send.at[peer, side], t3_recv.at[tp, side], t3_s.at[peer, side], t3_r.at[tp, side],
                {"tp": peer}))

    def scatter(side):
        total = t3_send[tp, side].astype(F32)
        for d in range(1, n_tp):
            peer = lax.rem(tp + d, n_tp)
            pltpu.make_async_remote_copy(
                src_ref=t3_send.at[peer, side], dst_ref=t3_recv.at[peer, side],
                send_sem=t3_s.at[peer, side], recv_sem=t3_r.at[peer, side],
                device_id={"tp": peer}, device_id_type=MESH).wait_recv()
            total = total + t3_recv[peer, side].astype(F32)
        mq[0, side] = total
        for c in range(n_chip):
            f_send[2 * c + side] = mq[0, side, c * seqs : (c + 1) * seqs, :].astype(BF16)
        for d in range(n_chip):
            to = 2 * lax.rem(chip + d, n_chip) + side
            if d or side is not core:
                pending.append(send(f_send.at[to], f_recv.at[dp], f_s.at[to], f_r.at[dp], {"dp": to}))
            else:
                pltpu.make_async_copy(f_send.at[dp], f_recv.at[dp], loc_sem.at[0]).start()

    project(core)
    for d in range(n_chip):
        recv_g(other, d)
    project(other)
    scatter(core)
    scatter(other)
    pltpu.make_async_copy(f_send.at[dp], f_recv.at[dp], loc_sem.at[0]).wait()
    for d in range(1, n_dp):
        peer = lax.rem(dp + d, n_dp)
        pltpu.make_async_remote_copy(
            src_ref=f_send.at[peer], dst_ref=f_recv.at[peer], send_sem=f_s.at[peer], recv_sem=f_r.at[peer],
            device_id={"dp": peer}, device_id_type=MESH).wait_recv()
    for r in range(n_dp):
        block = slice(r * ocols, (r + 1) * ocols)
        fin[:, block] = fin[:, block] + f_recv[r].astype(F32)
    resid = fin[...]
    inverse = lax.rsqrt(jnp.sum(resid * resid, axis=1, keepdims=True) / width + F32(1e-06))
    weighted = resid * gain[...]
    peak = jnp.max(jnp.abs(weighted), axis=1, keepdims=True)
    scale = (peak * inverse + F32(1e-06)) / F32(448.0)
    scaled = (weighted * (inverse / scale)).astype(BF16)
    for q in range(n_tp):
        o_send[q, 0] = resid[:, q * owide : (q + 1) * owide].astype(BF16)
        o_send[q, 1] = scaled[:, q * owide : (q + 1) * owide]
    spread = jnp.where(lane_i == row_i + tp * seqs, jnp.broadcast_to(scale, lane_i.shape), F32(0.0))
    c_send[...] = jnp.broadcast_to(jnp.sum(spread, axis=0, keepdims=True), c_send.shape)
    for d in range(1, n_tp):
        peer = lax.rem(tp + d, n_tp)
        pending.append(send(c_send, c_recv.at[tp], c_s.at[peer], c_r.at[tp], {"tp": peer}))
    pending += exchange(o_send, o_recv, o_s, o_r, lambda q: None)
    scales = c_send[...]
    for d in range(1, n_tp):
        peer = lax.rem(tp + d, n_tp)
        pltpu.make_async_remote_copy(
            src_ref=c_send, dst_ref=c_recv.at[peer], send_sem=c_s.at[peer], recv_sem=c_r.at[peer],
            device_id={"tp": peer}, device_id_type=MESH).wait_recv()
        scales = scales + c_recv[peer]
    scale_out[...] = scales
    for part, out in ((0, resid_out), (1, scaled_out)):
        for q in range(n_tp):
            b_rows[q * seqs : (q + 1) * seqs, :] = o_recv[q, part].astype(F32)
        out[...] = b_rows[...].astype(BF16)
    for copy in pending:
        copy.wait_send()


def finish(resid, scaled, scale, resid_out, scaled_out, scale_out):
    resid_out[...] = resid[...]
    scaled_out[...] = scaled[...]
    scale_out[...] = scale[0:1, : scale_out.shape[1]]


def fused(n_dp, n_tp, hidden, w_qkv, w_out, norm_gain, kv_cache, lengths):
    rows, width = hidden.shape
    seqs, kvh, ctx, hd2 = kv_cache.shape
    hd = hd2 // 2
    depth, cols = w_qkv.shape
    odepth, ocols = w_out.shape
    heads = odepth * n_tp // hd
    owide = width // n_tp
    chips = n_dp // 2
    vm = pltpu.VMEM
    dma = pltpu.SemaphoreType.DMA
    all_rows = seqs * heads
    scratch = [
        vm((2, chips, rows, depth), BF16), vm((depth, cols), BF16), vm((odepth, ocols), BF16),
        vm(kv_cache.shape, BF16), vm((rows, width), BF16), vm((rows, width), F32),
        vm((chips, rows, cols), BF16), vm((chips, rows, cols), BF16), vm((chips, rows, cols), F32),
        vm((chips, rows, cols), BF16), vm((chips, rows, cols), BF16), vm((rows, cols), F32),
        vm((n_tp, seqs, cols), BF16), vm((n_tp, seqs, cols), BF16),
        vm((all_rows, hd), F32), vm((all_rows, hd), F32), vm((all_rows, hd), F32), vm((all_rows, hd), F32),
        vm((all_rows, ctx), F32), vm((all_rows, hd), F32),
        vm((n_tp, seqs, odepth), BF16), vm((n_tp, seqs, odepth), BF16), vm((rows, odepth), F32),
        vm((2, chips, rows, odepth), BF16), vm((2, chips, rows, ocols), F32),
        vm((n_tp, 2, chips * seqs, ocols), F32), vm((n_tp, 2, chips * seqs, ocols), BF16),
        vm((n_tp, 2, chips * seqs, ocols), BF16),
        vm((n_dp, seqs, ocols), BF16), vm((n_dp, seqs, ocols), BF16),
        vm((n_tp, 2, seqs, owide), BF16), vm((n_tp, 2, seqs, owide), BF16),
        vm((8, hd), F32), vm((n_tp, 8, hd), F32), vm((seqs, width), F32),
        dma((5,)), dma((n_dp,)), dma((n_dp,)), dma, dma, dma((chips,)), dma((chips,)),
        dma((n_tp,)), dma((n_tp,)), dma((n_tp,)), dma((n_tp,)),
        dma((chips,)), dma((2, chips)), dma((chips,)), dma((n_tp, 2)), dma((n_tp, 2)),
        dma((n_dp,)), dma((n_dp,)), dma((n_tp,)), dma((n_tp,)), dma((n_tp,)), dma((n_tp,)),
    ]
    anywhere = pl.BlockSpec(memory_space=pl.ANY)
    in_vmem = pl.BlockSpec(memory_space=pltpu.VMEM)
    resid, scaled, scale = pl.pallas_call(
        functools.partial(layer, n_dp, n_tp),
        out_shape=(
            jax.ShapeDtypeStruct((rows, owide), BF16),
            jax.ShapeDtypeStruct((rows, owide), BF16),
            jax.ShapeDtypeStruct((8, hd), F32),
        ),
        in_specs=[anywhere, anywhere, anywhere, in_vmem, anywhere, pl.BlockSpec(memory_space=pltpu.SMEM)],
        out_specs=(in_vmem, in_vmem, in_vmem),
        scratch_shapes=scratch,
        compiler_params=pltpu.CompilerParams(
            collective_id=0, has_side_effects=True, vmem_limit_bytes=66_000_000),
    )(hidden, w_qkv, w_out, norm_gain.reshape(1, width), kv_cache, lengths)
    resid, scaled, scale = pl.pallas_call(
        finish,
        out_shape=(
            jax.ShapeDtypeStruct((rows, owide), BF16),
            jax.ShapeDtypeStruct((rows, owide), BF16),
            jax.ShapeDtypeStruct((1, rows), F32),
        ),
        in_specs=[in_vmem, in_vmem, in_vmem],
        out_specs=(in_vmem, in_vmem, in_vmem),
    )(resid, scaled, scale)
    return resid, scaled, scale.reshape(rows)


def solution(mesh):
    placed = (
        P("dp", None),
        P("dp", "tp"),
        P("tp", "dp"),
        P(),
        P(("dp", "tp"), None, None, None),
        P(("dp", "tp")),
    )
    n_dp, n_tp = mesh.shape["dp"], mesh.shape["tp"]

    def body(hidden, w_qkv, w_out, norm_gain, kv_cache, lengths):
        lanes = kv_cache.shape[3] // 2
        fits = (
            n_dp % 2 == 0
            and kv_cache.shape[2] == lanes
            and w_qkv.shape[1] % lanes == 0
            and w_out.shape[0] % lanes == 0
            and w_out.shape[1] % lanes == 0
            and hidden.shape[0] <= lanes
            and hidden.shape[1] // n_tp == w_out.shape[0]
        )
        if fits:
            return fused(n_dp, n_tp, hidden, w_qkv, w_out, norm_gain, kv_cache, lengths)
        return shards(hidden, w_qkv, w_out, norm_gain, kv_cache, lengths)

    return jax.shard_map(
        body,
        mesh=mesh,
        in_specs=placed,
        out_specs=(P("dp", "tp"), P("dp", "tp"), P("dp")),
        check_vma=False,
    )
```
